32 devices in a mesh: seq: 8 (over z, y), dp: 4 (over x, core).
Axes of the slice: x: 2, y: 2, z: 4, core: 2. Of those that a mesh axis runs over, the one named last changes fastest.
Arguments:
- queries: bfloat16 [8192, 2048], P(('dp', 'seq')), parts along dimension 0, may hold values from -5 to 5
- keys: bfloat16 [8192, 128], P(('dp', 'seq')), parts along dimension 0, may hold values from -5 to 5
- values: bfloat16 [8192, 128], P(('dp', 'seq')), parts along dimension 0, may hold values from -5 to 5
- lengths: int32 [32], P('dp'), parts along dimension 0, may hold values from 1 to 1024, 2048 in all
- grad_out: bfloat16 [8192, 2048], P(('dp', 'seq')), parts along dimension 0, may hold values from -5 to 5
Outputs:
- attended: bfloat16 [8192, 2048], P(('dp', 'seq')), parts along dimension 0
- grad_queries: bfloat16 [8192, 2048], P(('dp', 'seq')), parts along dimension 0
- grad_keys: bfloat16 [8192, 128], P(('dp', 'seq')), parts along dimension 0
- grad_values: bfloat16 [8192, 128], P(('dp', 'seq')), parts along dimension 0
The draws below stay inside these ranges and needn't reach their ends.
There are 4 independent parts, one for each index of `dp`. The reference program is written for one: setup_inputs(seed, part) draws one part's arguments, and reference() takes and returns one part's arrays. A program takes and returns all parts, laid end to end along the dimension named above; each array names one. Nothing has to cross between parts.
Inputs may be any that keep to these rules, and one draw needn't show every extreme that they name: The lengths sum to 2048.
All inputs are finite; a program needn't handle non-finite values.
Results may differ from the reference program's by a relative error of at most 0.018.
Values may be sent and summed in bfloat16 or wider, within the bound.
No kernel may reach another device: no remote copies, remote signals or barrier semaphores. Data moves between devices by JAX's collectives and lax.ppermute only.
A program may use at most 256 MiB of HBM per device.

```python
import math
import jax
import jax.numpy as jnp
import numpy as np
from jax import lax

H = 16
DH = 128
TOK_DEV = 256
SPAN = 4
MAXLEN = 1024
TOKENS = 2048
DOCS = 8
N_SEQ = 8


def draw_queries(key, part):
    noise = jnp.clip(jax.random.normal(jax.random.fold_in(key, 11), (TOKENS, H * DH), jnp.float32), -4.0, 4.0)
    return noise.astype(jnp.bfloat16)


def draw_keys(key, part):
    noise = jnp.clip(jax.random.normal(jax.random.fold_in(key, 21), (TOKENS, DH), jnp.float32), -4.0, 4.0)
    return noise.astype(jnp.bfloat16)


def steps_of(stream_key, dims, pieces, least, high):
    def one(dim, parts):
        draws = jax.random.uniform(jax.random.fold_in(jax.random.fold_in(stream_key, 6), dim), (parts,), jnp.float32, least / len(pieces), high / len(pieces))
        return jnp.repeat(jnp.exp(draws), dims[dim] // parts).reshape((-1,) + (1,) * (len(dims) - dim - 1))

    factor_of = one(*pieces[0])
    for cut in pieces[1:]:
        factor_of = factor_of * one(*cut)
    return factor_of


def length_profile(count, total, limit, skew):
    portions = [(1 << 20) // math.isqrt(grade ** skew) + 1 for grade in range(2, count + 1)]
    surplus, holding = total - limit - (count - 1), [1] * (count - 1)
    while surplus > 0:
        candidates = [i for i in range(count - 1) if holding[i] < limit]
        pool, budget = sum([portions[i] for i in candidates]), surplus
        for i in candidates:
            extra = min(limit - holding[i], max(1, budget * portions[i] // pool), surplus)
            holding[i] = holding[i] + extra
            surplus = surplus - extra
    return np.array([limit] + holding)


def uneven_parts(rng, number_of, total, limit, slope):
    if number_of == 2:
        one = jax.random.randint(rng, (), max(1, total - limit), min(limit, total - 1) + 1)
        return jnp.stack([one, total - one])
    sizes = jnp.asarray(length_profile(number_of, total, limit, slope), jnp.int32)
    twos = (number_of - 1) // 2
    source_of, sink = sizes[1:1 + 2 * twos:2], sizes[2:2 + 2 * twos:2]
    margin = jnp.minimum(source_of - 1, limit - sink)
    shifted = jax.random.randint(jax.random.fold_in(rng, 1), (twos,), 0, 1 << 20) % (margin + 1)
    sizes = sizes.at[1:1 + 2 * twos:2].set(source_of - shifted).at[2:2 + 2 * twos:2].set(sink + shifted)
    return sizes[jax.random.permutation(jax.random.fold_in(rng, 2), number_of)]


def gaussian(rng, shape, scale, bound, shards=(), kind=jnp.bfloat16):
    gain = steps_of(rng, shape, shards, -0.22, 0.18) if shards else 1.0
    entries = jax.random.normal(rng, shape, jnp.float32) * scale * gain
    return jnp.minimum(jnp.maximum(entries, -bound), bound).astype(kind)


def setup_inputs(seed: int = 0, part: int = 0) -> dict:
    seeds = jax.random.split(jax.random.key(seed), 6)
    part_splits = jax.random.split(jax.random.fold_in(seeds[5], part), 6)
    return {
        "queries": draw_queries(jax.random.fold_in(jax.random.fold_in(seeds[5], part), 71), part),
        "keys": draw_keys(jax.random.fold_in(jax.random.fold_in(seeds[5], part), 71), part),
        "values": gaussian(part_splits[2], (TOKENS, DH), 1.0, 5.0, ((0, 8),)),
        "lengths": uneven_parts(part_splits[3], DOCS, TOKENS, MAXLEN, 2).astype(jnp.int32),
        "grad_out": gaussian(part_splits[4], (TOKENS, H * DH), 1.0, 5.0, ((0, 8),)),
    }


NEG_FILL = -1.0e30


def reference(queries, keys, values, lengths, grad_out):
    score_scale = 1.0 / (DH ** 0.5)
    window_rows = (SPAN + 1) * TOK_DEV
    pad_rows = SPAN * TOK_DEV
    key_value = jnp.concatenate([keys, values], axis=1)
    padded = jnp.concatenate([jnp.zeros((pad_rows, 2 * DH), key_value.dtype), key_value], axis=0)
    doc_ends = jnp.cumsum(lengths).astype(jnp.int32)

    def one_block(grad_acc, block):
        first = (block * TOK_DEV).astype(jnp.int32)
        positions = first + jnp.arange(TOK_DEV, dtype=jnp.int32)
        doc_starts = jnp.max(jnp.where(doc_ends[None, :] <= positions[:, None], doc_ends[None, :], 0), axis=1)
        key_pos = first - pad_rows + jnp.arange(window_rows, dtype=jnp.int32)
        visible = (key_pos[None, :] >= doc_starts[:, None]) & (key_pos[None, :] <= positions[:, None])
        visible = jnp.broadcast_to(visible[:, None, :], (TOK_DEV, H, window_rows)).reshape(TOK_DEV * H, window_rows)
        section = lax.dynamic_slice_in_dim(padded, first, window_rows, 0)
        key_block = section[:, :DH]
        value_block = section[:, DH:]
        query_rows = lax.dynamic_slice_in_dim(queries, first, TOK_DEV, 0).reshape(TOK_DEV * H, DH)
        grad_rows = lax.dynamic_slice_in_dim(grad_out, first, TOK_DEV, 0).reshape(TOK_DEV * H, DH)
        scores = jnp.dot(query_rows, key_block.T, preferred_element_type=jnp.float32) * score_scale
        scores = jnp.where(visible, scores, NEG_FILL)
        top = jnp.max(scores, axis=1)
        total = jnp.sum(jnp.where(visible, jnp.exp(scores - top[:, None]), 0.0), axis=1)
        log_total = top + jnp.log(total)
        weights = jnp.where(visible, jnp.exp(scores - log_total[:, None]), 0.0)
        rounded = weights.astype(jnp.bfloat16)
        out_rows = jnp.dot(rounded, value_block, preferred_element_type=jnp.float32).astype(jnp.bfloat16)
        delta = jnp.sum(grad_rows.astype(jnp.float32) * out_rows.astype(jnp.float32), axis=1)
        grad_weights = jnp.dot(grad_rows, value_block.T, preferred_element_type=jnp.float32)
        grad_scores = (weights * (grad_weights - delta[:, None])).astype(jnp.bfloat16)
        grad_query = (score_scale * jnp.dot(grad_scores, key_block, preferred_element_type=jnp.float32)).astype(jnp.bfloat16)
        block_grad = jnp.concatenate([
            jnp.dot(grad_scores.T, query_rows, preferred_element_type=jnp.float32),
            jnp.dot(rounded.T, grad_rows, preferred_element_type=jnp.float32)], axis=1)
        current = lax.dynamic_slice_in_dim(grad_acc, first, window_rows, 0)
        grad_acc = lax.dynamic_update_slice_in_dim(grad_acc, current + block_grad, first, 0)
        return grad_acc, (out_rows.reshape(TOK_DEV, H * DH), grad_query.reshape(TOK_DEV, H * DH))

    start_acc = jnp.zeros((pad_rows + TOKENS, 2 * DH), jnp.float32)
    grad_acc, (outs, grads) = lax.scan(one_block, start_acc, jnp.arange(N_SEQ, dtype=jnp.int32))
    key_total = grad_acc[pad_rows:]
    attended = outs.reshape(TOKENS, H * DH)
    grad_queries = grads.reshape(TOKENS, H * DH)
    grad_keys = (score_scale * key_total[:, :DH]).astype(jnp.bfloat16)
    grad_values = key_total[:, DH:].astype(jnp.bfloat16)
    return (attended, grad_queries, grad_keys, grad_values)
```

```python
import functools
import math

import jax
import jax.numpy as jnp
from jax import lax
from jax.experimental import pallas as pl
from jax.experimental.pallas import tpu as pltpu
from jax.sharding import PartitionSpec as P

NEG_FILL = -1e30
LOG2_E = 1.4426950408889634


def passed_along(value, axis, steps):
    count = lax.axis_size(axis)
    first, last = (max(0, -steps), min(count, count - steps))
    return lax.ppermute(value, axis, [(source, source + steps) for source in range(first, last)])


def dot_nt(left, right):
    return lax.dot_general(left, right, (((1,), (1,)), ((), ())), preferred_element_type=jnp.float32)


def dot_nn(left, right):
    return lax.dot_general(left, right, (((1,), (0,)), ((), ())), preferred_element_type=jnp.float32)


def attention_kernel(
    slot_count,
    head_count,
    score_scale,
    start_ref,
    q_ref,
    qt_ref,
    g_ref,
    gt_ref,
    kv_ref,
    out_ref,
    dq_ref,
    grad_ref,
    bias_ref,
    vext_ref,
):
    tokens = q_ref.shape[0]
    width = kv_ref.shape[2] // 2
    factor = score_scale * LOG2_E
    row_start = start_ref[...]
    for slot in range(slot_count):
        key_pos = lax.broadcasted_iota(jnp.int32, (tokens, tokens), 1) - slot * tokens
        visible = key_pos >= row_start
        if slot == 0:
            visible = visible & (key_pos <= lax.broadcasted_iota(jnp.int32, (tokens, tokens), 0))
        bias_ref[slot] = jnp.where(visible, 0.0, NEG_FILL)
        vext_ref[slot, :, :width] = kv_ref[slot, :, width:]
        vext_ref[slot, :, width:] = jnp.ones((tokens, width), jnp.bfloat16)
        grad_ref[slot] = jnp.zeros((2 * width, tokens), jnp.float32)

    def one_head(head, carry):
        lanes = pl.ds(pl.multiple_of(head * width, width), width)
        q = q_ref[:, lanes]
        g = g_ref[:, lanes]
        qt = qt_ref[lanes, :]
        gt = gt_ref[lanes, :]
        scores = []
        top = None
        for slot in range(slot_count):
            s = dot_nt(q, kv_ref[slot, :, :width]) * factor + bias_ref[slot]
            scores.append(s)
            top = s if top is None else jnp.maximum(top, s)
        top = jnp.max(top, axis=1, keepdims=True)
        weights = []
        acc = None
        for slot in range(slot_count):
            w = jnp.exp2(scores[slot] - top).astype(jnp.bfloat16)
            weights.append(w)
            part = dot_nn(w, vext_ref[slot])
            acc = part if acc is None else acc + part
        inverse = 1.0 / acc[:, width:]
        out = (acc[:, :width] * inverse).astype(jnp.bfloat16)
        out_ref[:, lanes] = out
        delta = jnp.sum(g.astype(jnp.float32) * out.astype(jnp.float32), axis=1, keepdims=True)
        inverse = jnp.concatenate([inverse] * (tokens // width), axis=1)
        dq = None
        for slot in range(slot_count):
            dp = dot_nt(g, kv_ref[slot, :, width:])
            w = weights[slot].astype(jnp.float32) * inverse
            ds = (w * (dp - delta)).astype(jnp.bfloat16)
            part = dot_nn(ds, kv_ref[slot, :, :width])
            dq = part if dq is None else dq + part
            grad_ref[slot, :width] += dot_nn(qt, ds)
            grad_ref[slot, width:] += dot_nn(gt, w.astype(jnp.bfloat16))
        dq_ref[:, lanes] = (score_scale * dq).astype(jnp.bfloat16)
        return carry

    lax.fori_loop(0, head_count, one_head, 0)


def local_math(start, q, qt, g, gt, kv, head_count, score_scale):
    slot_count, tokens, both = kv.shape
    vmem = pl.BlockSpec(memory_space=pltpu.VMEM)
    return pl.pallas_call(
        functools.partial(attention_kernel, slot_count, head_count, score_scale),
        out_shape=(
            jax.ShapeDtypeStruct(q.shape, jnp.bfloat16),
            jax.ShapeDtypeStruct(q.shape, jnp.bfloat16),
            jax.ShapeDtypeStruct((slot_count, both, tokens), jnp.float32),
        ),
        in_specs=[vmem] * 6,
        out_specs=(vmem, vmem, vmem),
        scratch_shapes=[
            pltpu.VMEM((slot_count, tokens, tokens), jnp.float32),
            pltpu.VMEM((slot_count, tokens, both), jnp.bfloat16),
        ],
        compiler_params=pltpu.CompilerParams(vmem_limit_bytes=40 << 20),
        name="attention",
    )(start, q, qt, g, gt, kv)


def shards(queries, keys, values, lengths, grad_out):
    tokens = queries.shape[0]
    width = keys.shape[1]
    head_count = queries.shape[1] // width
    axis_size = lax.axis_size("seq")
    reach = min(8, axis_size // 2)
    rank = lax.axis_index("seq")
    score_scale = 1.0 / math.sqrt(width)

    own = jnp.concatenate([keys, values], axis=1)
    far = [passed_along(own, "seq", 1)]
    if reach > 1:
        far.append(passed_along(own, "seq", 2))
    window = jnp.stack(far)
    while window.shape[0] < reach:
        window = jnp.concatenate([window, passed_along(window, "seq", window.shape[0])], axis=0)
    window = jnp.concatenate([own[None], window], axis=0)

    first = rank * tokens
    positions = first + jnp.arange(tokens, dtype=jnp.int32)
    doc_ends = jnp.cumsum(lengths)
    starts = jnp.max(jnp.where(doc_ends[None, :] <= positions[:, None], doc_ends[None, :], 0), axis=1)
    starts = (starts - first).astype(jnp.int32)[:, None]

    out, dq, grads = local_math(
        starts, queries, queries.T, grad_out, grad_out.T, window, head_count, score_scale
    )
    total = grads[0]
    rest = grads[1:]
    while rest.shape[0] > 2:
        half = rest.shape[0] // 2
        moved = passed_along(rest[half:].astype(jnp.bfloat16), "seq", -half)
        rest = rest[:half] + moved.astype(jnp.float32)
    for offset in range(rest.shape[0]):
        moved = passed_along(rest[offset].astype(jnp.bfloat16), "seq", -1 - offset)
        total = total + moved.astype(jnp.float32)
    grad_keys = (score_scale * total[:width]).astype(jnp.bfloat16).T
    grad_values = total[width:].astype(jnp.bfloat16).T
    return (out, dq, grad_keys, grad_values)


def solution(mesh):
    rows = P(("dp", "seq"), None)
    return jax.shard_map(
        shards,
        mesh=mesh,
        in_specs=(rows, rows, rows, P("dp"), rows),
        out_specs=(rows, rows, rows, rows),
        check_vma=False,
    )
```

```python
import functools
import math

import jax
import jax.numpy as jnp
from jax import lax
from jax.experimental import pallas as pl
from jax.experimental.pallas import tpu as pltpu
from jax.sharding import PartitionSpec as P

NEG_FILL = -1e30
LOG2_E = 1.4426950408889634


def ring_shift(value, steps):
    count = lax.axis_size("seq")
    return lax.ppermute(value, "seq", [(i, (i + steps) % count) for i in range(count)])


def dot_nt(left, right):
    return lax.dot_general(left, right, (((1,), (1,)), ((), ())), preferred_element_type=jnp.float32)


def dot_nn(left, right):
    return lax.dot_general(left, right, (((1,), (0,)), ((), ())), preferred_element_type=jnp.float32)


def head_lanes(head, width):
    return pl.ds(pl.multiple_of(head * width, width), width)


def take_rows(ref, group, pack, width):
    heads = [ref[:, head_lanes(group * pack + i, width)] for i in range(pack)]
    return jnp.concatenate(heads, axis=0)


def take_columns(ref, group, pack, width):
    heads = [ref[head_lanes(group * pack + i, width), :] for i in range(pack)]
    return jnp.concatenate(heads, axis=1)


def put_rows(ref, group, pack, width, value):
    tokens = value.shape[0] // pack
    for i in range(pack):
        ref[:, head_lanes(group * pack + i, width)] = value[i * tokens : (i + 1) * tokens]


def split_chain(lefts, rights, parts):
    step = lefts[0].shape[0] // parts
    sums = [None] * parts
    for left, right in zip(lefts, rights):
        for i in range(parts):
            part = dot_nn(left[i * step : (i + 1) * step], right)
            sums[i] = part if sums[i] is None else sums[i] + part
    return jnp.concatenate(sums, axis=0)


def row_dots(left, right):
    return jnp.sum(left.astype(jnp.float32) * right.astype(jnp.float32), axis=1, keepdims=True)


def backward_group(group, pack, width, g, delta, slots, q_t, g_t, weights, kv_refs, grad_ref):
    tokens = kv_refs[0].shape[0] // 2
    steps = []
    for index, (w, kv_ref) in enumerate(zip(weights, kv_refs)):
        dp = dot_nt(g, kv_ref[tokens:])
        ds = (w.astype(jnp.float32) * (dp - delta)).astype(jnp.bfloat16)
        steps.append(ds)
        grad_ref[index, :width] += dot_nn(q_t, ds)
        grad_ref[index, width:] += dot_nn(g_t, w)
    return split_chain(steps, [kv_ref[:tokens] for kv_ref in kv_refs], 2)


def first_kernel(slot_count, near, pack, head_count, score_scale, *refs):
    start_ref, q_ref, qt_ref, g_ref, gt_ref = refs[:5]
    kv_refs = refs[5 : 5 + slot_count]
    out_ref, dq_ref, grad_out_ref, kept_ref, bias_ref, vext_ref, grad_ref = refs[5 + slot_count :]
    tokens = q_ref.shape[0]
    width = q_ref.shape[1] // head_count
    rows = pack * tokens
    factor = score_scale * LOG2_E
    row_start = start_ref[...]
    for slot in range(slot_count):
        key_pos = lax.broadcasted_iota(jnp.int32, (tokens, tokens), 1) - slot * tokens
        visible = key_pos >= row_start
        if slot == 0:
            visible = visible & (key_pos <= lax.broadcasted_iota(jnp.int32, (tokens, tokens), 0))
        bias_ref[slot] = jnp.where(visible, 0.0, NEG_FILL)
        vext_ref[slot, :, :width] = kv_refs[slot][tokens:]
        vext_ref[slot, :, width:] = jnp.ones((tokens, width), jnp.bfloat16)
    grad_ref[...] = jnp.zeros(grad_ref.shape, jnp.float32)

    def one_group(group, carry):
        q = take_rows(q_ref, group, pack, width)
        g = take_rows(g_ref, group, pack, width)
        scores = []
        top = None
        for slot in range(slot_count):
            s = dot_nt(q, kv_refs[slot][:tokens]).reshape(pack, tokens, tokens)
            s = (s * factor + bias_ref[slot][None]).reshape(rows, tokens)
            scores.append(s)
            top = s if top is None else jnp.maximum(top, s)
        top = jnp.max(top, axis=1, keepdims=True)
        weights = [jnp.exp2(s - top).astype(jnp.bfloat16) for s in scores]
        total = split_chain(weights, [vext_ref[slot] for slot in range(slot_count)], 2)
        inverse = 1.0 / total[:, width:]
        out = (total[:, :width] * inverse).astype(jnp.bfloat16)
        put_rows(out_ref, group, pack, width, out)
        delta = row_dots(g, out)
        inverse = jnp.concatenate([inverse] * (tokens // width), axis=1)
        weights = [(w.astype(jnp.float32) * inverse).astype(jnp.bfloat16) for w in weights]
        group_rows = pl.ds(pl.multiple_of(group * rows, rows), rows)
        for slot in range(near):
            kept_ref[slot, group_rows] = weights[slot]
        q_t = take_columns(qt_ref, group, pack, width)
        g_t = take_columns(gt_ref, group, pack, width)
        dq = backward_group(
            group, pack, width, g, delta, slot_count, q_t, g_t, weights[near:], kv_refs[near:], grad_ref
        )
        put_rows(dq_ref, group, pack, width, dq)
        return carry

    lax.fori_loop(0, head_count // pack, one_group, 0)
    grad_out_ref[...] = grad_ref[...].astype(grad_out_ref.dtype)


def later_kernel(first_slot, slots, pack, head_count, dq_scale, *refs):
    qt_ref, g_ref, gt_ref, out_ref, kept_ref, dq_in_ref = refs[:6]
    kv_refs = refs[6 : 6 + slots]
    dq_ref, grad_ref = refs[6 + slots :]
    tokens = g_ref.shape[0]
    width = g_ref.shape[1] // head_count
    rows = pack * tokens
    grad_ref[...] = jnp.zeros(grad_ref.shape, jnp.float32)

    def one_group(group, carry):
        g = take_rows(g_ref, group, pack, width)
        delta = row_dots(g, take_rows(out_ref, group, pack, width))
        group_rows = pl.ds(pl.multiple_of(group * rows, rows), rows)
        weights = [kept_ref[first_slot + index, group_rows] for index in range(slots)]
        q_t = take_columns(qt_ref, group, pack, width)
        g_t = take_columns(gt_ref, group, pack, width)
        dq = backward_group(
            group, pack, width, g, delta, slots, q_t, g_t, weights, kv_refs, grad_ref
        )
        dq = dq + take_rows(dq_in_ref, group, pack, width)
        put_rows(dq_ref, group, pack, width, (dq * dq_scale).astype(dq_ref.dtype))
        return carry

    lax.fori_loop(0, head_count // pack, one_group, 0)


VMEM = pl.BlockSpec(memory_space=pltpu.VMEM)


def first_call(start, q, qt, g, gt, kvs, near, pack, head_count, score_scale):
    slot_count = len(kvs)
    tokens = q.shape[0]
    width = q.shape[1] // head_count
    far = slot_count - near
    return pl.pallas_call(
        functools.partial(first_kernel, slot_count, near, pack, head_count, score_scale),
        out_shape=(
            jax.ShapeDtypeStruct(q.shape, jnp.bfloat16),
            jax.ShapeDtypeStruct(q.shape, jnp.float32),
            jax.ShapeDtypeStruct((far, 2 * width, tokens), jnp.bfloat16),
            jax.ShapeDtypeStruct((near, head_count * tokens, tokens), jnp.bfloat16),
        ),
        in_specs=[VMEM] * (5 + slot_count),
        out_specs=(VMEM,) * 4,
        scratch_shapes=[
            pltpu.VMEM((slot_count, tokens, tokens), jnp.float32),
            pltpu.VMEM((slot_count, tokens, 2 * width), jnp.bfloat16),
            pltpu.VMEM((far, 2 * width, tokens), jnp.float32),
        ],
        compiler_params=pltpu.CompilerParams(vmem_limit_bytes=40 << 20),
        name="forward_far",
    )(start, q, qt, g, gt, *kvs)


def later_call(qt, g, gt, out, kept, dq, kvs, first_slot, pack, head_count, dq_scale, last):
    slots = len(kvs)
    tokens = g.shape[0]
    width = g.shape[1] // head_count
    return pl.pallas_call(
        functools.partial(later_kernel, first_slot, slots, pack, head_count, dq_scale),
        out_shape=(
            jax.ShapeDtypeStruct(g.shape, jnp.bfloat16 if last else jnp.float32),
            jax.ShapeDtypeStruct((slots, 2 * width, tokens), jnp.float32),
        ),
        in_specs=[VMEM] * (6 + slots),
        out_specs=(VMEM,) * 2,
        compiler_params=pltpu.CompilerParams(vmem_limit_bytes=24 << 20),
        name="backward_near",
    )(qt, g, gt, out, kept, dq, *kvs)


def shards(queries, keys, values, lengths, grad_out):
    tokens = queries.shape[0]
    width = keys.shape[1]
    head_count = queries.shape[1] // width
    reach = min(8, lax.axis_size("seq") // 2)
    rank = lax.axis_index("seq")
    score_scale = 1.0 / math.sqrt(width)
    pack = math.gcd(8, head_count)

    own = jnp.concatenate([keys, values], axis=0)
    window = [own]
    if reach > 1:
        two = ring_shift(own, 2)
        one = ring_shift(own, 1)
        window += [one, two]
    else:
        window += [ring_shift(own, 1)]
    if reach > 2:
        four = ring_shift(two, 2)
        three = ring_shift(two, 1)
        window += [three, four]
    while len(window) <= reach:
        shift = len(window) - 1
        window += [ring_shift(part, shift) for part in window[1:]]

    first = rank * tokens
    positions = first + jnp.arange(tokens, dtype=jnp.int32)
    doc_ends = jnp.cumsum(lengths)
    starts = jnp.max(jnp.where(doc_ends[None, :] <= positions[:, None], doc_ends[None, :], 0), axis=1)
    starts = (starts - first).astype(jnp.int32)[:, None]
    queries_t, grads_t = queries.T, grad_out.T

    near = reach // 2 + 1
    out, dq, far_grads, kept = first_call(
        starts, queries, queries_t, grad_out, grads_t, window, near, pack, head_count, score_scale
    )
    moved = ring_shift(far_grads, -(reach // 2))
    dq, near_grads = later_call(
        queries_t, grad_out, grads_t, out, kept, dq, window[1:near], 1, pack, head_count, 1.0, False
    )
    near_grads = (near_grads + moved.astype(jnp.float32)).astype(jnp.bfloat16)
    while near_grads.shape[0] > 2:
        half = near_grads.shape[0] // 2
        back = ring_shift(near_grads[half:], -half)
        near_grads = (near_grads[:half].astype(jnp.float32) + back.astype(jnp.float32)).astype(jnp.bfloat16)
    received = [ring_shift(near_grads[i], -1 - i) for i in range(near_grads.shape[0])]
    dq, own_grads = later_call(
        queries_t, grad_out, grads_t, out, kept, dq, window[:1], 0, pack, head_count, score_scale, True
    )
    total = own_grads[0]
    for part in received:
        total = total + part.astype(jnp.float32)
    grad_keys = (score_scale * total[:width]).astype(jnp.bfloat16).T
    grad_values = total[width:].astype(jnp.bfloat16).T
    return (out, dq, grad_keys, grad_values)


def solution(mesh):
    rows = P(("dp", "seq"), None)
    return jax.shard_map(
        shards,
        mesh=mesh,
        in_specs=(rows, rows, rows, P("dp"), rows),
        out_specs=(rows, rows, rows, rows),
        check_vma=False,
    )
```

```python
import functools
import math

import jax
import jax.numpy as jnp
from jax import lax
from jax.experimental import pallas as pl
from jax.experimental.pallas import tpu as pltpu
from jax.sharding import PartitionSpec as P

NEG_FILL = -1e30
LOG2_E = 1.4426950408889634


def ring_shift(value, steps):
    count = lax.axis_size("seq")
    return lax.ppermute(value, "seq", [(i, (i + steps) % count) for i in range(count)])


def dot_nt(left, right):
    return lax.dot_general(left, right, (((1,), (1,)), ((), ())), preferred_element_type=jnp.float32)


def dot_nn(left, right):
    return lax.dot_general(left, right, (((1,), (0,)), ((), ())), preferred_element_type=jnp.float32)


def head_lanes(head, width):
    return pl.ds(pl.multiple_of(head * width, width), width)


def take_rows(ref, group, pack, width):
    heads = [ref[:, head_lanes(group * pack + i, width)] for i in range(pack)]
    return jnp.concatenate(heads, axis=0)


def take_columns(ref, group, pack, width):
    heads = [ref[head_lanes(group * pack + i, width), :] for i in range(pack)]
    return jnp.concatenate(heads, axis=1)


def put_rows(ref, group, pack, width, value):
    tokens = value.shape[0] // pack
    for i in range(pack):
        ref[:, head_lanes(group * pack + i, width)] = value[i * tokens : (i + 1) * tokens]


def split_chain(lefts, rights, parts):
    step = lefts[0].shape[0] // parts
    sums = [None] * parts
    for left, right in zip(lefts, rights):
        for i in range(parts):
            part = dot_nn(left[i * step : (i + 1) * step], right)
            sums[i] = part if sums[i] is None else sums[i] + part
    return jnp.concatenate(sums, axis=0)


def row_dots(left, right):
    return jnp.sum(left.astype(jnp.float32) * right.astype(jnp.float32), axis=1, keepdims=True)


def backward_group(group, pack, width, g, delta, slots, q_t, g_t, weights, kv_refs, grad_ref):
    tokens = kv_refs[0].shape[0] // 2
    steps = []
    for index, (w, kv_ref) in enumerate(zip(weights, kv_refs)):
        dp = dot_nt(g, kv_ref[tokens:])
        ds = (w.astype(jnp.float32) * (dp - delta)).astype(jnp.bfloat16)
        steps.append(ds)
        grad_ref[index, :width] += dot_nn(q_t, ds)
        grad_ref[index, width:] += dot_nn(g_t, w)
    return split_chain(steps, [kv_ref[:tokens] for kv_ref in kv_refs], 2)


def join_kernel(keys_ref, values_ref, own_ref, sems):
    tokens = keys_ref.shape[0]
    copies = [
        pltpu.make_async_copy(keys_ref, own_ref.at[pl.ds(0, tokens)], sems.at[0]),
        pltpu.make_async_copy(values_ref, own_ref.at[pl.ds(tokens, tokens)], sems.at[1]),
    ]
    for copy in copies:
        copy.start()
    for copy in copies:
        copy.wait()


def prepare_kernel(
    slot_count, lengths_ref, q_in, g_in, q_ref, g_ref, qt_ref, gt_ref, bias_ref, sems
):
    tokens = q_ref.shape[0]
    copies = [
        pltpu.make_async_copy(q_in, q_ref, sems.at[0]),
        pltpu.make_async_copy(g_in, g_ref, sems.at[1]),
    ]
    for copy in copies:
        copy.start()
    first = lax.axis_index("seq") * tokens
    row = lax.broadcasted_iota(jnp.int32, (tokens, tokens), 0)
    lane = lax.broadcasted_iota(jnp.int32, (tokens, tokens), 1)
    row_start = jnp.full((tokens, tokens), -first, jnp.int32)
    end = -first
    for document in range(lengths_ref.shape[0]):
        end = end + lengths_ref[document]
        row_start = jnp.where(row >= end, end, row_start)
    for slot in range(slot_count):
        visible = lane - slot * tokens >= row_start
        if slot == 0:
            visible = visible & (lane <= row)
        bias_ref[slot] = jnp.where(visible, 0.0, NEG_FILL)
    copies[0].wait()
    qt_ref[...] = q_ref[...].T
    copies[1].wait()
    gt_ref[...] = g_ref[...].T


def finish_kernel(score_scale, own_ref, *refs):
    part_refs, (keys_ref, values_ref) = refs[:-2], refs[-2:]
    width = keys_ref.shape[1]
    total = own_ref[0]
    for part_ref in part_refs:
        total = total + part_ref[...].astype(jnp.float32)
    keys_ref[...] = (score_scale * total[:width]).T.astype(jnp.bfloat16)
    values_ref[...] = total[width:].T.astype(jnp.bfloat16)


def first_kernel(slot_count, near, pack, head_count, score_scale, *refs):
    bias_ref, q_ref, qt_ref, g_ref, gt_ref = refs[:5]
    kv_refs = refs[5 : 5 + slot_count]
    out_ref, dq_ref, grad_out_ref, kept_ref, delta_ref, vext_ref, grad_ref = refs[5 + slot_count :]
    tokens = q_ref.shape[0]
    width = q_ref.shape[1] // head_count
    rows = pack * tokens
    factor = score_scale * LOG2_E
    for slot in range(slot_count):
        vext_ref[slot, :, :width] = kv_refs[slot][tokens:]
        vext_ref[slot, :, width:] = jnp.ones((tokens, width), jnp.bfloat16)
    grad_ref[...] = jnp.zeros(grad_ref.shape, jnp.float32)

    def one_group(group, carry):
        q = take_rows(q_ref, group, pack, width)
        g = take_rows(g_ref, group, pack, width)
        scores = []
        top = None
        for slot in range(slot_count):
            s = dot_nt(q, kv_refs[slot][:tokens]).reshape(pack, tokens, tokens)
            s = (s * factor + bias_ref[slot][None]).reshape(rows, tokens)
            scores.append(s)
            top = s if top is None else jnp.maximum(top, s)
        top = jnp.max(top, axis=1, keepdims=True)
        weights = [jnp.exp2(s - top).astype(jnp.bfloat16) for s in scores]
        total = split_chain(weights, [vext_ref[slot] for slot in range(slot_count)], 2)
        inverse = 1.0 / total[:, width:]
        out = (total[:, :width] * inverse).astype(jnp.bfloat16)
        put_rows(out_ref, group, pack, width, out)
        delta = row_dots(g, out)
        inverse = jnp.concatenate([inverse] * (tokens // width), axis=1)
        weights = [(w.astype(jnp.float32) * inverse).astype(jnp.bfloat16) for w in weights]
        group_rows = pl.ds(pl.multiple_of(group * rows, rows), rows)
        delta_ref[group_rows] = jnp.broadcast_to(delta, (rows, width))
        for slot in range(near):
            kept_ref[slot, group_rows] = weights[slot]
        q_t = take_columns(qt_ref, group, pack, width)
        g_t = take_columns(gt_ref, group, pack, width)
        dq = backward_group(
            group, pack, width, g, delta, slot_count, q_t, g_t, weights[near:], kv_refs[near:], grad_ref
        )
        put_rows(dq_ref, group, pack, width, dq)
        return carry

    lax.fori_loop(0, head_count // pack, one_group, 0)
    grad_out_ref[...] = grad_ref[...].astype(grad_out_ref.dtype)


def later_kernel(first_slot, slots, pack, head_count, dq_scale, *refs):
    qt_ref, g_ref, gt_ref, delta_ref, kept_ref, dq_in_ref = refs[:6]
    kv_refs = refs[6 : 6 + slots]
    dq_ref, grad_ref = refs[6 + slots :]
    tokens = g_ref.shape[0]
    width = g_ref.shape[1] // head_count
    rows = pack * tokens
    grad_ref[...] = jnp.zeros(grad_ref.shape, jnp.float32)

    def one_group(group, carry):
        g = take_rows(g_ref, group, pack, width)
        group_rows = pl.ds(pl.multiple_of(group * rows, rows), rows)
        delta = jnp.concatenate([delta_ref[group_rows]] * (tokens // width), axis=1)
        weights = [kept_ref[first_slot + index, group_rows] for index in range(slots)]
        q_t = take_columns(qt_ref, group, pack, width)
        g_t = take_columns(gt_ref, group, pack, width)
        dq = backward_group(
            group, pack, width, g, delta, slots, q_t, g_t, weights, kv_refs, grad_ref
        )
        dq = dq + take_rows(dq_in_ref, group, pack, width)
        put_rows(dq_ref, group, pack, width, (dq * dq_scale).astype(dq_ref.dtype))
        return carry

    lax.fori_loop(0, head_count // pack, one_group, 0)


VMEM = pl.BlockSpec(memory_space=pltpu.VMEM)
HBM = pl.BlockSpec(memory_space=pltpu.HBM)


def in_hbm(value):
    return pltpu.with_memory_space_constraint(value, pltpu.HBM)


def join_call(keys, values):
    return pl.pallas_call(
        join_kernel,
        out_shape=jax.ShapeDtypeStruct((2 * keys.shape[0], keys.shape[1]), keys.dtype),
        in_specs=[HBM] * 2,
        out_specs=VMEM,
        scratch_shapes=[pltpu.SemaphoreType.DMA((2,))],
        compiler_params=pltpu.CompilerParams(vmem_limit_bytes=1 << 20),
        name="join",
    )(in_hbm(keys), in_hbm(values))


def prepare_call(lengths, q, g, slot_count):
    tokens, lanes = q.shape
    return pl.pallas_call(
        functools.partial(prepare_kernel, slot_count),
        out_shape=(
            jax.ShapeDtypeStruct(q.shape, q.dtype),
            jax.ShapeDtypeStruct(g.shape, g.dtype),
            jax.ShapeDtypeStruct((lanes, tokens), q.dtype),
            jax.ShapeDtypeStruct((lanes, tokens), g.dtype),
            jax.ShapeDtypeStruct((slot_count, tokens, tokens), jnp.float32),
        ),
        in_specs=[pl.BlockSpec(memory_space=pltpu.SMEM), HBM, HBM],
        out_specs=(VMEM,) * 5,
        scratch_shapes=[pltpu.SemaphoreType.DMA((2,))],
        compiler_params=pltpu.CompilerParams(vmem_limit_bytes=2 << 20),
        name="prepare",
    )(in_hbm(lengths), in_hbm(q), in_hbm(g))


def finish_call(own, parts, score_scale, width):
    tokens = own.shape[2]
    shape = jax.ShapeDtypeStruct((tokens, width), jnp.bfloat16)
    return pl.pallas_call(
        functools.partial(finish_kernel, score_scale),
        out_shape=(shape, shape),
        in_specs=[VMEM] * (1 + len(parts)),
        out_specs=(VMEM,) * 2,
        compiler_params=pltpu.CompilerParams(vmem_limit_bytes=1 << 20),
        name="finish",
    )(own, *parts)


def first_call(bias, q, qt, g, gt, kvs, near, pack, head_count, score_scale):
    slot_count = len(kvs)
    tokens = q.shape[0]
    width = q.shape[1] // head_count
    far = slot_count - near
    return pl.pallas_call(
        functools.partial(first_kernel, slot_count, near, pack, head_count, score_scale),
        out_shape=(
            jax.ShapeDtypeStruct(q.shape, jnp.bfloat16),
            jax.ShapeDtypeStruct(q.shape, jnp.float32),
            jax.ShapeDtypeStruct((far, 2 * width, tokens), jnp.bfloat16),
            jax.ShapeDtypeStruct((near, head_count * tokens, tokens), jnp.bfloat16),
            jax.ShapeDtypeStruct((head_count * tokens, width), jnp.float32),
        ),
        in_specs=[VMEM] * (5 + slot_count),
        out_specs=(VMEM,) * 5,
        scratch_shapes=[
            pltpu.VMEM((slot_count, tokens, 2 * width), jnp.bfloat16),
            pltpu.VMEM((far, 2 * width, tokens), jnp.float32),
        ],
        compiler_params=pltpu.CompilerParams(vmem_limit_bytes=slot_count * (5 << 20)),
        name="forward_far",
    )(bias, q, qt, g, gt, *kvs)


def later_call(qt, g, gt, delta, kept, dq, kvs, first_slot, pack, head_count, dq_scale, last):
    slots = len(kvs)
    tokens = g.shape[0]
    width = g.shape[1] // head_count
    return pl.pallas_call(
        functools.partial(later_kernel, first_slot, slots, pack, head_count, dq_scale),
        out_shape=(
            jax.ShapeDtypeStruct(g.shape, jnp.bfloat16 if last else jnp.float32),
            jax.ShapeDtypeStruct((slots, 2 * width, tokens), jnp.float32),
        ),
        in_specs=[VMEM] * (6 + slots),
        out_specs=(VMEM,) * 2,
        compiler_params=pltpu.CompilerParams(vmem_limit_bytes=slots * (3 << 20)),
        name="backward_near",
    )(qt, g, gt, delta, kept, dq, *kvs)


def shards(queries, keys, values, lengths, grad_out):
    width = keys.shape[1]
    head_count = queries.shape[1] // width
    reach = min(8, lax.axis_size("seq") // 2)
    score_scale = 1.0 / math.sqrt(width)
    pack = math.gcd(8, head_count)

    own = join_call(keys, values)
    window = [own]
    if reach > 1:
        two = ring_shift(own, 2)
        one = ring_shift(own, 1)
        window += [one, two]
    else:
        window += [ring_shift(own, 1)]
    if reach > 2:
        four = ring_shift(two, 2)
        three = ring_shift(two, 1)
        window += [three, four]
    while len(window) <= reach:
        shift = len(window) - 1
        window += [ring_shift(part, shift) for part in window[1:]]

    queries, grad_out, queries_t, grads_t, bias = prepare_call(
        lengths, queries, grad_out, reach + 1
    )

    near = reach // 2 + 1
    out, dq, far_grads, kept, delta = first_call(
        bias, queries, queries_t, grad_out, grads_t, window, near, pack, head_count, score_scale
    )
    moved = ring_shift(far_grads, -(reach // 2))
    dq, near_grads = later_call(
        queries_t, grad_out, grads_t, delta, kept, dq, window[1:near], 1, pack, head_count, 1.0, False
    )
    near_grads = (near_grads + moved.astype(jnp.float32)).astype(jnp.bfloat16)
    while near_grads.shape[0] > 2:
        half = near_grads.shape[0] // 2
        back = ring_shift(near_grads[half:], -half)
        near_grads = (near_grads[:half].astype(jnp.float32) + back.astype(jnp.float32)).astype(jnp.bfloat16)
    received = [ring_shift(near_grads[i], -1 - i) for i in range(near_grads.shape[0])]
    dq, own_grads = later_call(
        queries_t, grad_out, grads_t, delta, kept, dq, window[:1], 0, pack, head_count, score_scale, True
    )
    grad_keys, grad_values = finish_call(own_grads, received, score_scale, width)
    return (out, dq, grad_keys, grad_values)


def solution(mesh):
    rows = P(("dp", "seq"), None)
    return jax.shard_map(
        shards,
        mesh=mesh,
        in_specs=(rows, rows, rows, P("dp"), rows),
        out_specs=(rows, rows, rows, rows),
        check_vma=False,
    )
```

```python
import functools
import math

import jax
import jax.numpy as jnp
from jax import lax
from jax.experimental import pallas as pl
from jax.experimental.pallas import tpu as pltpu
from jax.sharding import PartitionSpec as P

NEG_FILL = -1e30
LOG2_E = 1.4426950408889634


def ring_shift(value, steps):
    count = lax.axis_size("seq")
    return lax.ppermute(value, "seq", [(i, (i + steps) % count) for i in range(count)])


def dot_nt(left, right):
    return lax.dot_general(left, right, (((1,), (1,)), ((), ())), preferred_element_type=jnp.float32)


def dot_nn(left, right):
    return lax.dot_general(left, right, (((1,), (0,)), ((), ())), preferred_element_type=jnp.float32)


def head_lanes(head, width):
    return pl.ds(pl.multiple_of(head * width, width), width)


def take_rows(ref, group, pack, width):
    heads = [ref[:, head_lanes(group * pack + i, width)] for i in range(pack)]
    return jnp.concatenate(heads, axis=0)


def take_columns(ref, group, pack, width):
    heads = [ref[head_lanes(group * pack + i, width), :] for i in range(pack)]
    return jnp.concatenate(heads, axis=1)


def put_rows(ref, group, pack, width, value):
    tokens = value.shape[0] // pack
    for i in range(pack):
        ref[:, head_lanes(group * pack + i, width)] = value[i * tokens : (i + 1) * tokens]


def split_chain(lefts, rights, parts):
    step = lefts[0].shape[0] // parts
    sums = [None] * parts
    for left, right in zip(lefts, rights):
        for i in range(parts):
            part = dot_nn(left[i * step : (i + 1) * step], right)
            sums[i] = part if sums[i] is None else sums[i] + part
    return jnp.concatenate(sums, axis=0)


def row_dots(left, right):
    return jnp.sum(left.astype(jnp.float32) * right.astype(jnp.float32), axis=1, keepdims=True)


def backward_group(g, delta, q_t, g_t, weights, kv_refs, grad_ref):
    tokens, width = kv_refs[0].shape[0] // 2, kv_refs[0].shape[1]
    steps = []
    for index, (w, kv_ref) in enumerate(zip(weights, kv_refs)):
        dp = dot_nt(g, kv_ref[tokens:])
        ds = (w.astype(jnp.float32) * (dp - delta)).astype(jnp.bfloat16)
        steps.append(ds)
        grad_ref[index, :width] += dot_nn(q_t, ds)
        grad_ref[index, width:] += dot_nn(g_t, w)
    return split_chain(steps, [kv_ref[:tokens] for kv_ref in kv_refs], 2)


def join_kernel(keys_ref, values_ref, own_ref, sems):
    tokens = keys_ref.shape[0]
    copies = [
        pltpu.make_async_copy(keys_ref, own_ref.at[pl.ds(0, tokens)], sems.at[0]),
        pltpu.make_async_copy(values_ref, own_ref.at[pl.ds(tokens, tokens)], sems.at[1]),
    ]
    for copy in copies:
        copy.start()
    for copy in copies:
        copy.wait()


def prepare_kernel(
    slot_count, lengths_ref, q_in, g_in, q_ref, g_ref, qt_ref, gt_ref, bias_ref, sems
):
    tokens = q_ref.shape[0]
    copies = [
        pltpu.make_async_copy(q_in, q_ref, sems.at[0]),
        pltpu.make_async_copy(g_in, g_ref, sems.at[1]),
    ]
    for copy in copies:
        copy.start()
    first = lax.axis_index("seq") * tokens
    row = lax.broadcasted_iota(jnp.int32, (tokens, tokens), 0)
    lane = lax.broadcasted_iota(jnp.int32, (tokens, tokens), 1)
    row_start = jnp.full((tokens, tokens), -first, jnp.int32)
    end = -first
    for document in range(lengths_ref.shape[0]):
        end = end + lengths_ref[document]
        row_start = jnp.where(row >= end, end, row_start)
    for slot in range(slot_count):
        visible = lane - slot * tokens >= row_start
        if slot == 0:
            visible = visible & (lane <= row)
        bias_ref[slot] = jnp.where(visible, 0.0, NEG_FILL)
    copies[0].wait()
    qt_ref[...] = q_ref[...].T
    copies[1].wait()
    gt_ref[...] = g_ref[...].T


def finish_kernel(score_scale, own_ref, *refs):
    part_refs, (keys_ref, values_ref) = refs[:-2], refs[-2:]
    width = keys_ref.shape[1]
    total = own_ref[0]
    for part_ref in part_refs:
        total = total + part_ref[...].astype(jnp.float32)
    keys_ref[...] = (score_scale * total[:width]).T.astype(jnp.bfloat16)
    values_ref[...] = total[width:].T.astype(jnp.bfloat16)


def forward_slots(q, bias_ref, first_slot, kv_refs, vext_ref, factor, pack, top):
    rows = q.shape[0]
    tokens = rows // pack
    scores = []
    for index, kv_ref in enumerate(kv_refs):
        part = dot_nt(q, kv_ref[:tokens]).reshape(pack, tokens, tokens)
        part = (part * factor + bias_ref[first_slot + index][None]).reshape(rows, tokens)
        scores.append(part)
    highest = scores[0]
    for part in scores[1:]:
        highest = jnp.maximum(highest, part)
    highest = jnp.max(highest, axis=1, keepdims=True)
    if top is not None:
        highest = jnp.maximum(highest, top)
    weights = [jnp.exp2(part - highest).astype(jnp.bfloat16) for part in scores]
    total = split_chain(weights, [vext_ref[index] for index in range(len(kv_refs))], 2)
    return highest, weights, total


def extend_values(kv_refs, vext_ref):
    tokens, width = kv_refs[0].shape[0] // 2, kv_refs[0].shape[1]
    for index, kv_ref in enumerate(kv_refs):
        vext_ref[index, :, :width] = kv_ref[tokens:]
        vext_ref[index, :, width:] = jnp.ones((tokens, width), jnp.bfloat16)


def near_kernel(slots, pack, head_count, score_scale, *refs):
    bias_ref, q_ref = refs[:2]
    kv_refs = refs[2 : 2 + slots]
    kept_ref, total_ref, top_ref, vext_ref = refs[2 + slots :]
    width = q_ref.shape[1] // head_count
    rows = pack * q_ref.shape[0]
    extend_values(kv_refs, vext_ref)

    def one_group(group, carry):
        q = take_rows(q_ref, group, pack, width)
        top, weights, total = forward_slots(
            q, bias_ref, 0, kv_refs, vext_ref, score_scale * LOG2_E, pack, None
        )
        group_rows = pl.ds(pl.multiple_of(group * rows, rows), rows)
        for slot in range(slots):
            kept_ref[slot, group_rows] = weights[slot]
        total_ref[group_rows] = total
        top_ref[group_rows] = jnp.broadcast_to(top, (rows, width))
        return carry

    lax.fori_loop(0, head_count // pack, one_group, 0)


def far_kernel(first_slot, slots, pack, head_count, score_scale, *refs):
    bias_ref, q_ref, qt_ref, g_ref, gt_ref, total_ref, top_ref = refs[:7]
    kv_refs = refs[7 : 7 + slots]
    out_ref, dq_ref, grad_out_ref, rate_ref, delta_ref, vext_ref, grad_ref = refs[7 + slots :]
    tokens = q_ref.shape[0]
    width = q_ref.shape[1] // head_count
    rows = pack * tokens
    extend_values(kv_refs, vext_ref)
    grad_ref[...] = jnp.zeros(grad_ref.shape, jnp.float32)

    def one_group(group, carry):
        group_rows = pl.ds(pl.multiple_of(group * rows, rows), rows)
        q = take_rows(q_ref, group, pack, width)
        g = take_rows(g_ref, group, pack, width)
        near_top = top_ref[group_rows]
        top, weights, total = forward_slots(
            q, bias_ref, first_slot, kv_refs, vext_ref, score_scale * LOG2_E, pack, near_top[:, :1]
        )
        shrink = jnp.exp2(near_top - top)
        near_total = total_ref[group_rows]
        inverse = 1.0 / (near_total[:, width:] * shrink + total[:, width:])
        out = ((near_total[:, :width] * shrink + total[:, :width]) * inverse).astype(jnp.bfloat16)
        put_rows(out_ref, group, pack, width, out)
        delta = row_dots(g, out)
        delta_ref[group_rows] = jnp.broadcast_to(delta, (rows, width))
        rate_ref[group_rows] = shrink * inverse
        inverse = jnp.concatenate([inverse] * (tokens // width), axis=1)
        weights = [(w.astype(jnp.float32) * inverse).astype(jnp.bfloat16) for w in weights]
        q_t = take_columns(qt_ref, group, pack, width)
        g_t = take_columns(gt_ref, group, pack, width)
        dq = backward_group(g, delta, q_t, g_t, weights, kv_refs, grad_ref)
        put_rows(dq_ref, group, pack, width, dq)
        return carry

    lax.fori_loop(0, head_count // pack, one_group, 0)
    grad_out_ref[...] = grad_ref[...].astype(grad_out_ref.dtype)


def later_kernel(first_slot, slots, pack, head_count, dq_scale, *refs):
    qt_ref, g_ref, gt_ref, rate_ref, delta_ref, kept_ref, dq_in_ref = refs[:7]
    kv_refs = refs[7 : 7 + slots]
    dq_ref, grad_ref = refs[7 + slots :]
    tokens = g_ref.shape[0]
    width = g_ref.shape[1] // head_count
    rows = pack * tokens
    grad_ref[...] = jnp.zeros(grad_ref.shape, jnp.float32)

    def one_group(group, carry):
        g = take_rows(g_ref, group, pack, width)
        group_rows = pl.ds(pl.multiple_of(group * rows, rows), rows)
        delta = jnp.concatenate([delta_ref[group_rows]] * (tokens // width), axis=1)
        rate = jnp.concatenate([rate_ref[group_rows]] * (tokens // width), axis=1)
        weights = [
            (kept_ref[first_slot + index, group_rows].astype(jnp.float32) * rate).astype(jnp.bfloat16)
            for index in range(slots)
        ]
        q_t = take_columns(qt_ref, group, pack, width)
        g_t = take_columns(gt_ref, group, pack, width)
        dq = backward_group(g, delta, q_t, g_t, weights, kv_refs, grad_ref)
        dq = dq + take_rows(dq_in_ref, group, pack, width)
        put_rows(dq_ref, group, pack, width, (dq * dq_scale).astype(dq_ref.dtype))
        return carry

    lax.fori_loop(0, head_count // pack, one_group, 0)


VMEM = pl.BlockSpec(memory_space=pltpu.VMEM)
HBM = pl.BlockSpec(memory_space=pltpu.HBM)


def in_hbm(value):
    return pltpu.with_memory_space_constraint(value, pltpu.HBM)


def join_call(keys, values):
    return pl.pallas_call(
        join_kernel,
        out_shape=jax.ShapeDtypeStruct((2 * keys.shape[0], keys.shape[1]), keys.dtype),
        in_specs=[HBM] * 2,
        out_specs=VMEM,
        scratch_shapes=[pltpu.SemaphoreType.DMA((2,))],
        compiler_params=pltpu.CompilerParams(vmem_limit_bytes=1 << 20),
        name="join",
    )(in_hbm(keys), in_hbm(values))


def prepare_call(lengths, q, g, slot_count):
    tokens, lanes = q.shape
    return pl.pallas_call(
        functools.partial(prepare_kernel, slot_count),
        out_shape=(
            jax.ShapeDtypeStruct(q.shape, q.dtype),
            jax.ShapeDtypeStruct(g.shape, g.dtype),
            jax.ShapeDtypeStruct((lanes, tokens), q.dtype),
            jax.ShapeDtypeStruct((lanes, tokens), g.dtype),
            jax.ShapeDtypeStruct((slot_count, tokens, tokens), jnp.float32),
        ),
        in_specs=[pl.BlockSpec(memory_space=pltpu.SMEM), HBM, HBM],
        out_specs=(VMEM,) * 5,
        scratch_shapes=[pltpu.SemaphoreType.DMA((2,))],
        compiler_params=pltpu.CompilerParams(vmem_limit_bytes=2 << 20),
        name="prepare",
    )(in_hbm(lengths), in_hbm(q), in_hbm(g))


def finish_call(own, parts, score_scale, width):
    tokens = own.shape[2]
    shape = jax.ShapeDtypeStruct((tokens, width), jnp.bfloat16)
    return pl.pallas_call(
        functools.partial(finish_kernel, score_scale),
        out_shape=(shape, shape),
        in_specs=[VMEM] * (1 + len(parts)),
        out_specs=(VMEM,) * 2,
        compiler_params=pltpu.CompilerParams(vmem_limit_bytes=1 << 20),
        name="finish",
    )(own, *parts)


def near_call(bias, q, kvs, pack, head_count, score_scale):
    slots = len(kvs)
    tokens = q.shape[0]
    width = q.shape[1] // head_count
    rows = head_count * tokens
    return pl.pallas_call(
        functools.partial(near_kernel, slots, pack, head_count, score_scale),
        out_shape=(
            jax.ShapeDtypeStruct((slots, rows, tokens), jnp.bfloat16),
            jax.ShapeDtypeStruct((rows, 2 * width), jnp.float32),
            jax.ShapeDtypeStruct((rows, width), jnp.float32),
        ),
        in_specs=[VMEM] * (2 + slots),
        out_specs=(VMEM,) * 3,
        scratch_shapes=[pltpu.VMEM((slots, tokens, 2 * width), jnp.bfloat16)],
        compiler_params=pltpu.CompilerParams(vmem_limit_bytes=(slots + 1) * (4 << 20)),
        name="forward_near",
    )(bias, q, *kvs)


def far_call(bias, q, qt, g, gt, total, top, kvs, first_slot, pack, head_count, score_scale):
    slots = len(kvs)
    tokens = q.shape[0]
    width = q.shape[1] // head_count
    rows = head_count * tokens
    return pl.pallas_call(
        functools.partial(far_kernel, first_slot, slots, pack, head_count, score_scale),
        out_shape=(
            jax.ShapeDtypeStruct(q.shape, jnp.bfloat16),
            jax.ShapeDtypeStruct(q.shape, jnp.float32),
            jax.ShapeDtypeStruct((slots, 2 * width, tokens), jnp.bfloat16),
            jax.ShapeDtypeStruct((rows, width), jnp.float32),
            jax.ShapeDtypeStruct((rows, width), jnp.float32),
        ),
        in_specs=[VMEM] * (7 + slots),
        out_specs=(VMEM,) * 5,
        scratch_shapes=[
            pltpu.VMEM((slots, tokens, 2 * width), jnp.bfloat16),
            pltpu.VMEM((slots, 2 * width, tokens), jnp.float32),
        ],
        compiler_params=pltpu.CompilerParams(vmem_limit_bytes=(slots + 1) * (5 << 20)),
        name="forward_far",
    )(bias, q, qt, g, gt, total, top, *kvs)


def later_call(qt, g, gt, rate, delta, kept, dq, kvs, first_slot, pack, head_count, dq_scale, last):
    slots = len(kvs)
    tokens = g.shape[0]
    width = g.shape[1] // head_count
    return pl.pallas_call(
        functools.partial(later_kernel, first_slot, slots, pack, head_count, dq_scale),
        out_shape=(
            jax.ShapeDtypeStruct(g.shape, jnp.bfloat16 if last else jnp.float32),
            jax.ShapeDtypeStruct((slots, 2 * width, tokens), jnp.float32),
        ),
        in_specs=[VMEM] * (7 + slots),
        out_specs=(VMEM,) * 2,
        compiler_params=pltpu.CompilerParams(vmem_limit_bytes=slots * (3 << 20)),
        name="backward_near",
    )(qt, g, gt, rate, delta, kept, dq, *kvs)


def shards(queries, keys, values, lengths, grad_out):
    width = keys.shape[1]
    head_count = queries.shape[1] // width
    reach = min(8, lax.axis_size("seq") // 2)
    score_scale = 1.0 / math.sqrt(width)
    pack = math.gcd(8, head_count)

    near = reach // 2 + 1
    own = join_call(keys, values)
    two = ring_shift(own, 2)
    one = ring_shift(own, 1)
    queries, grad_out, queries_t, grads_t, bias = prepare_call(
        lengths, queries, grad_out, reach + 1
    )
    two, bias = lax.optimization_barrier((two, bias))
    window = [own, one, two]
    if reach > 2:
        window += [ring_shift(two, 1), ring_shift(two, 2)]
    while len(window) <= reach:
        shift = len(window) - 1
        window += [ring_shift(part, shift) for part in window[1:]]
    window = window[: reach + 1]

    kept, total, top = near_call(bias, queries, window[:near], pack, head_count, score_scale)
    out, dq, far_grads, rate, delta = far_call(
        bias, queries, queries_t, grad_out, grads_t, total, top, window[near:], near, pack, head_count, score_scale
    )
    moved = ring_shift(far_grads, -(reach // 2))
    dq, near_grads = later_call(
        queries_t, grad_out, grads_t, rate, delta, kept, dq, window[1:near], 1, pack, head_count, 1.0, False
    )
    near_grads = (near_grads + moved.astype(jnp.float32)).astype(jnp.bfloat16)
    while near_grads.shape[0] > 2:
        half = near_grads.shape[0] // 2
        back = ring_shift(near_grads[half:], -half)
        near_grads = (near_grads[:half].astype(jnp.float32) + back.astype(jnp.float32)).astype(jnp.bfloat16)
    received = [ring_shift(near_grads[i], -1 - i) for i in range(near_grads.shape[0])]
    dq, own_grads = later_call(
        queries_t, grad_out, grads_t, rate, delta, kept, dq, window[:1], 0, pack, head_count, score_scale, True
    )
    grad_keys, grad_values = finish_call(own_grads, received, score_scale, width)
    return (out, dq, grad_keys, grad_values)


def solution(mesh):
    rows = P(("dp", "seq"), None)
    return jax.shard_map(
        shards,
        mesh=mesh,
        in_specs=(rows, rows, rows, P("dp"), rows),
        out_specs=(rows, rows, rows, rows),
        check_vma=False,
    )
```

```python
import functools
import math

import jax
import jax.numpy as jnp
from jax import lax
from jax.experimental import pallas as pl
from jax.experimental.pallas import tpu as pltpu
from jax.sharding import PartitionSpec as P

NEG_FILL = -1e30
LOG2_E = 1.4426950408889634


def ring_shift(value, steps):
    count = lax.axis_size("seq")
    return lax.ppermute(value, "seq", [(i, (i + steps) % count) for i in range(count)])


def dot_nt(left, right):
    return lax.dot_general(left, right, (((1,), (1,)), ((), ())), preferred_element_type=jnp.float32)


def dot_nn(left, right):
    return lax.dot_general(left, right, (((1,), (0,)), ((), ())), preferred_element_type=jnp.float32)


def head_lanes(head, width):
    return pl.ds(pl.multiple_of(head * width, width), width)


def take_rows(ref, group, pack, width):
    heads = [ref[:, head_lanes(group * pack + i, width)] for i in range(pack)]
    return jnp.concatenate(heads, axis=0)


def take_columns(ref, group, pack, width):
    heads = [ref[head_lanes(group * pack + i, width), :] for i in range(pack)]
    return jnp.concatenate(heads, axis=1)


def put_rows(ref, group, pack, width, value):
    tokens = value.shape[0] // pack
    for i in range(pack):
        ref[:, head_lanes(group * pack + i, width)] = value[i * tokens : (i + 1) * tokens]


def split_chain(lefts, rights, parts):
    step = lefts[0].shape[0] // parts
    sums = [None] * parts
    for left, right in zip(lefts, rights):
        for i in range(parts):
            part = dot_nn(left[i * step : (i + 1) * step], right)
            sums[i] = part if sums[i] is None else sums[i] + part
    return jnp.concatenate(sums, axis=0)


def split_nt(left, right, parts):
    step = left.shape[0] // parts
    return jnp.concatenate([dot_nt(left[i * step : (i + 1) * step], right) for i in range(parts)], axis=0)


def row_dots(left, right):
    return jnp.sum(left.astype(jnp.float32) * right.astype(jnp.float32), axis=1, keepdims=True)


def backward_slots(g, delta, q_t, g_t, weights, kv_refs, grad_ref, parts):
    tokens, width = kv_refs[0].shape[0] // 2, kv_refs[0].shape[1]
    steps = []
    for index, (w, kv_ref) in enumerate(zip(weights, kv_refs)):
        dp = split_nt(g, kv_ref[tokens:], parts)
        ds = (w.astype(jnp.float32) * (dp - delta)).astype(jnp.bfloat16)
        steps.append(ds)
        grad_ref[index, :width] += dot_nn(q_t, ds)
        grad_ref[index, width:] += dot_nn(g_t, w)
    return steps


def join_kernel(keys_ref, values_ref, own_ref, sems):
    tokens = keys_ref.shape[0]
    copies = [
        pltpu.make_async_copy(keys_ref, own_ref.at[pl.ds(0, tokens)], sems.at[0]),
        pltpu.make_async_copy(values_ref, own_ref.at[pl.ds(tokens, tokens)], sems.at[1]),
    ]
    for copy in copies:
        copy.start()
    for copy in copies:
        copy.wait()


def prepare_kernel(
    slot_count, lengths_ref, q_in, g_in, q_ref, g_ref, qt_ref, gt_ref, bias_ref, sems
):
    tokens = q_ref.shape[0]
    copies = [
        pltpu.make_async_copy(q_in, q_ref, sems.at[0]),
        pltpu.make_async_copy(g_in, g_ref, sems.at[1]),
    ]
    for copy in copies:
        copy.start()
    first = lax.axis_index("seq") * tokens
    row = lax.broadcasted_iota(jnp.int32, (tokens, tokens), 0)
    lane = lax.broadcasted_iota(jnp.int32, (tokens, tokens), 1)
    row_start = jnp.full((tokens, tokens), -first, jnp.int32)
    end = -first
    for document in range(lengths_ref.shape[0]):
        end = end + lengths_ref[document]
        row_start = jnp.where(row >= end, end, row_start)
    for slot in range(slot_count):
        visible = lane - slot * tokens >= row_start
        if slot == 0:
            visible = visible & (lane <= row)
        bias_ref[slot] = jnp.where(visible, 0.0, NEG_FILL)
    copies[0].wait()
    qt_ref[...] = q_ref[...].T
    copies[1].wait()
    gt_ref[...] = g_ref[...].T


def finish_kernel(score_scale, own_ref, *refs):
    part_refs, (keys_ref, values_ref) = refs[:-2], refs[-2:]
    width = keys_ref.shape[1]
    total = own_ref[0]
    for part_ref in part_refs:
        total = total + part_ref[...].astype(jnp.float32)
    keys_ref[...] = (score_scale * total[:width]).T.astype(jnp.bfloat16)
    values_ref[...] = total[width:].T.astype(jnp.bfloat16)


def forward_slots(q, bias_ref, first_slot, kv_refs, vext_ref, factor, pack, top):
    rows = q.shape[0]
    tokens = rows // pack
    scores = []
    for index, kv_ref in enumerate(kv_refs):
        part = dot_nt(q, kv_ref[:tokens]).reshape(pack, tokens, tokens)
        part = (part * factor + bias_ref[first_slot + index][None]).reshape(rows, tokens)
        scores.append(part)
    highest = scores[0]
    for part in scores[1:]:
        highest = jnp.maximum(highest, part)
    highest = jnp.broadcast_to(jnp.max(highest, axis=1, keepdims=True), (rows, q.shape[1]))
    if top is not None:
        highest = jnp.maximum(highest, top)
    level = jnp.concatenate([highest] * (tokens // q.shape[1]), axis=1)
    weights = [jnp.exp2(part - level).astype(jnp.bfloat16) for part in scores]
    total = split_chain(weights, [vext_ref[index] for index in range(len(kv_refs))], 2)
    return highest, weights, total


def extend_values(kv_refs, vext_ref):
    tokens, width = kv_refs[0].shape[0] // 2, kv_refs[0].shape[1]
    for index, kv_ref in enumerate(kv_refs):
        vext_ref[index, :, :width] = kv_ref[tokens:]
        vext_ref[index, :, width:] = jnp.ones((tokens, width), jnp.bfloat16)


def near_kernel(slots, pack, head_count, score_scale, *refs):
    bias_ref, q_ref = refs[:2]
    kv_refs = refs[2 : 2 + slots]
    kept_ref, total_ref, top_ref, vext_ref = refs[2 + slots :]
    width = q_ref.shape[1] // head_count
    rows = pack * q_ref.shape[0]
    extend_values(kv_refs, vext_ref)

    def one_group(group, carry):
        q = take_rows(q_ref, group, pack, width)
        top, weights, total = forward_slots(
            q, bias_ref, 0, kv_refs, vext_ref, score_scale * LOG2_E, pack, None
        )
        group_rows = pl.ds(pl.multiple_of(group * rows, rows), rows)
        for slot in range(slots):
            kept_ref[slot, group_rows] = weights[slot]
        total_ref[group_rows] = total
        top_ref[group_rows] = top
        return carry

    lax.fori_loop(0, head_count // pack, one_group, 0)


def far_kernel(first_slot, slots, pack, head_count, score_scale, *refs):
    bias_ref, q_ref, qt_ref, g_ref, gt_ref, total_ref, top_ref = refs[:7]
    kv_refs = refs[7 : 7 + slots]
    out_ref, step_ref, grad_out_ref, rate_ref, delta_ref, vext_ref, grad_ref = refs[7 + slots :]
    tokens = q_ref.shape[0]
    width = q_ref.shape[1] // head_count
    rows = pack * tokens
    extend_values(kv_refs, vext_ref)
    grad_ref[...] = jnp.zeros(grad_ref.shape, jnp.float32)

    def one_group(group, carry):
        group_rows = pl.ds(pl.multiple_of(group * rows, rows), rows)
        q = take_rows(q_ref, group, pack, width)
        g = take_rows(g_ref, group, pack, width)
        near_top = top_ref[group_rows]
        top, weights, total = forward_slots(
            q, bias_ref, first_slot, kv_refs, vext_ref, score_scale * LOG2_E, pack, near_top
        )
        shrink = jnp.exp2(near_top - top)
        near_total = total_ref[group_rows]
        inverse = 1.0 / (near_total[:, width:] * shrink + total[:, width:])
        out = ((near_total[:, :width] * shrink + total[:, :width]) * inverse).astype(jnp.bfloat16)
        put_rows(out_ref, group, pack, width, out)
        delta = row_dots(g, out)
        delta_ref[group_rows] = jnp.broadcast_to(delta, (rows, width))
        rate_ref[group_rows] = shrink * inverse
        inverse = jnp.concatenate([inverse] * (tokens // width), axis=1)
        weights = [(w.astype(jnp.float32) * inverse).astype(jnp.bfloat16) for w in weights]
        q_t = take_columns(qt_ref, group, pack, width)
        g_t = take_columns(gt_ref, group, pack, width)
        steps = backward_slots(g, delta, q_t, g_t, weights, kv_refs, grad_ref, 1)
        for slot in range(slots):
            step_ref[slot, group_rows] = steps[slot]
        return carry

    lax.fori_loop(0, head_count // pack, one_group, 0, unroll=True)
    grad_out_ref[...] = grad_ref[...].astype(grad_out_ref.dtype)


def later_kernel(first_slot, slots, pack, head_count, score_scale, *refs):
    qt_ref, g_ref, gt_ref, rate_ref, delta_ref, kept_ref = refs[:6]
    kv_refs = refs[6 : 6 + slots]
    last = first_slot == 0
    if last:
        step_refs = refs[6 + slots : 8 + slots]
        more_refs = refs[8 + slots : -2]
        dq_ref, grad_ref = refs[-2:]
    else:
        step_ref, grad_ref = refs[6 + slots :]
    tokens = g_ref.shape[0]
    width = g_ref.shape[1] // head_count
    rows = pack * tokens
    grad_ref[...] = jnp.zeros(grad_ref.shape, jnp.float32)

    def one_group(group, carry):
        g = take_rows(g_ref, group, pack, width)
        group_rows = pl.ds(pl.multiple_of(group * rows, rows), rows)
        delta = jnp.concatenate([delta_ref[group_rows]] * (tokens // width), axis=1)
        rate = jnp.concatenate([rate_ref[group_rows]] * (tokens // width), axis=1)
        weights = [
            (kept_ref[first_slot + index, group_rows].astype(jnp.float32) * rate).astype(jnp.bfloat16)
            for index in range(slots)
        ]
        q_t = take_columns(qt_ref, group, pack, width)
        g_t = take_columns(gt_ref, group, pack, width)
        steps = backward_slots(g, delta, q_t, g_t, weights, kv_refs, grad_ref, 2)
        if last:
            for held_ref in step_refs:
                steps = steps + [held_ref[slot, group_rows] for slot in range(held_ref.shape[0])]
            dq = split_chain(steps, [ref[:tokens] for ref in (*kv_refs, *more_refs)], 2)
            put_rows(dq_ref, group, pack, width, (dq * score_scale).astype(jnp.bfloat16))
        else:
            for slot in range(slots):
                step_ref[slot, group_rows] = steps[slot]
        return carry

    lax.fori_loop(0, head_count // pack, one_group, 0)


VMEM = pl.BlockSpec(memory_space=pltpu.VMEM)
HBM = pl.BlockSpec(memory_space=pltpu.HBM)


def in_hbm(value):
    return pltpu.with_memory_space_constraint(value, pltpu.HBM)


def join_call(keys, values):
    return pl.pallas_call(
        join_kernel,
        out_shape=jax.ShapeDtypeStruct((2 * keys.shape[0], keys.shape[1]), keys.dtype),
        in_specs=[HBM] * 2,
        out_specs=VMEM,
        scratch_shapes=[pltpu.SemaphoreType.DMA((2,))],
        compiler_params=pltpu.CompilerParams(vmem_limit_bytes=1 << 20),
        name="join",
    )(in_hbm(keys), in_hbm(values))


def prepare_call(lengths, q, g, slot_count):
    tokens, lanes = q.shape
    return pl.pallas_call(
        functools.partial(prepare_kernel, slot_count),
        out_shape=(
            jax.ShapeDtypeStruct(q.shape, q.dtype),
            jax.ShapeDtypeStruct(g.shape, g.dtype),
            jax.ShapeDtypeStruct((lanes, tokens), q.dtype),
            jax.ShapeDtypeStruct((lanes, tokens), g.dtype),
            jax.ShapeDtypeStruct((slot_count, tokens, tokens), jnp.float32),
        ),
        in_specs=[pl.BlockSpec(memory_space=pltpu.SMEM), HBM, HBM],
        out_specs=(VMEM,) * 5,
        scratch_shapes=[pltpu.SemaphoreType.DMA((2,))],
        compiler_params=pltpu.CompilerParams(vmem_limit_bytes=2 << 20),
        name="prepare",
    )(in_hbm(lengths), in_hbm(q), in_hbm(g))


def finish_call(own, parts, score_scale, width):
    tokens = own.shape[2]
    shape = jax.ShapeDtypeStruct((tokens, width), jnp.bfloat16)
    return pl.pallas_call(
        functools.partial(finish_kernel, score_scale),
        out_shape=(shape, shape),
        in_specs=[VMEM] * (1 + len(parts)),
        out_specs=(VMEM,) * 2,
        compiler_params=pltpu.CompilerParams(vmem_limit_bytes=1 << 20),
        name="finish",
    )(own, *parts)


def near_call(bias, q, kvs, pack, head_count, score_scale):
    slots = len(kvs)
    tokens = q.shape[0]
    width = q.shape[1] // head_count
    rows = head_count * tokens
    return pl.pallas_call(
        functools.partial(near_kernel, slots, pack, head_count, score_scale),
        out_shape=(
            jax.ShapeDtypeStruct((slots, rows, tokens), jnp.bfloat16),
            jax.ShapeDtypeStruct((rows, 2 * width), jnp.float32),
            jax.ShapeDtypeStruct((rows, width), jnp.float32),
        ),
        in_specs=[VMEM] * (2 + slots),
        out_specs=(VMEM,) * 3,
        scratch_shapes=[pltpu.VMEM((slots, tokens, 2 * width), jnp.bfloat16)],
        compiler_params=pltpu.CompilerParams(vmem_limit_bytes=(slots + 1) * (4 << 20)),
        name="forward_near",
    )(bias, q, *kvs)


def far_call(bias, q, qt, g, gt, total, top, kvs, first_slot, pack, head_count, score_scale):
    slots = len(kvs)
    tokens = q.shape[0]
    width = q.shape[1] // head_count
    rows = head_count * tokens
    return pl.pallas_call(
        functools.partial(far_kernel, first_slot, slots, pack, head_count, score_scale),
        out_shape=(
            jax.ShapeDtypeStruct(q.shape, jnp.bfloat16),
            jax.ShapeDtypeStruct((slots, rows, tokens), jnp.bfloat16),
            jax.ShapeDtypeStruct((slots, 2 * width, tokens), jnp.bfloat16),
            jax.ShapeDtypeStruct((rows, width), jnp.float32),
            jax.ShapeDtypeStruct((rows, width), jnp.float32),
        ),
        in_specs=[VMEM] * (7 + slots),
        out_specs=(VMEM,) * 5,
        scratch_shapes=[
            pltpu.VMEM((slots, tokens, 2 * width), jnp.bfloat16),
            pltpu.VMEM((slots, 2 * width, tokens), jnp.float32),
        ],
        compiler_params=pltpu.CompilerParams(vmem_limit_bytes=(slots + 1) * (7 << 20)),
        name="forward_far",
    )(bias, q, qt, g, gt, total, top, *kvs)


def later_call(qt, g, gt, rate, delta, kept, kvs, steps, more, first_slot, pack, head_count, score_scale):
    slots = len(kvs)
    tokens = g.shape[0]
    width = g.shape[1] // head_count
    if steps:
        result = jax.ShapeDtypeStruct(g.shape, jnp.bfloat16)
    else:
        result = jax.ShapeDtypeStruct((slots, head_count * tokens, tokens), jnp.bfloat16)
    return pl.pallas_call(
        functools.partial(later_kernel, first_slot, slots, pack, head_count, score_scale),
        out_shape=(result, jax.ShapeDtypeStruct((slots, 2 * width, tokens), jnp.float32)),
        in_specs=[VMEM] * (6 + slots + len(steps) + len(more)),
        out_specs=(VMEM,) * 2,
        compiler_params=pltpu.CompilerParams(vmem_limit_bytes=(slots + 1) * (4 << 20)),
        name="backward_last" if steps else "backward_near",
    )(qt, g, gt, rate, delta, kept, *kvs, *steps, *more)


def shards(queries, keys, values, lengths, grad_out):
    width = keys.shape[1]
    head_count = queries.shape[1] // width
    reach = min(8, lax.axis_size("seq") // 2)
    score_scale = 1.0 / math.sqrt(width)
    pack_a = math.gcd(8, head_count)
    pack_f = math.gcd(8, head_count)
    pack_2 = math.gcd(16, head_count)
    pack_3 = math.gcd(16, head_count)

    near = reach // 2 + 1
    own = join_call(keys, values)
    two = ring_shift(own, 2)
    one = ring_shift(own, 1)
    queries, grad_out, queries_t, grads_t, bias = prepare_call(
        lengths, queries, grad_out, reach + 1
    )
    two, bias = lax.optimization_barrier((two, bias))
    window = [own, one, two]
    if reach > 2:
        window += [ring_shift(two, 1), ring_shift(two, 2)]
    while len(window) <= reach:
        shift = len(window) - 1
        window += [ring_shift(part, shift) for part in window[1:]]
    window = window[: reach + 1]

    kept, total, top = near_call(bias, queries, window[:near], pack_a, head_count, score_scale)
    out, far_steps, far_grads, rate, delta = far_call(
        bias, queries, queries_t, grad_out, grads_t, total, top, window[near:], near, pack_f, head_count, score_scale
    )
    moved = ring_shift(far_grads, -(reach // 2))
    shared = (queries_t, grad_out, grads_t, rate, delta, kept)
    near_steps, near_grads = later_call(
        *shared, window[1:near], [], [], 1, pack_2, head_count, score_scale
    )
    near_grads = (near_grads + moved.astype(jnp.float32)).astype(jnp.bfloat16)
    while near_grads.shape[0] > 2:
        half = near_grads.shape[0] // 2
        back = ring_shift(near_grads[half:], -half)
        near_grads = (near_grads[:half].astype(jnp.float32) + back.astype(jnp.float32)).astype(jnp.bfloat16)
    received = [ring_shift(near_grads[i], -1 - i) for i in range(near_grads.shape[0])]
    dq, own_grads = later_call(
        *shared, window[:1], [near_steps, far_steps], window[1:], 0, pack_3, head_count, score_scale
    )
    grad_keys, grad_values = finish_call(own_grads, received, score_scale, width)
    return (out, dq, grad_keys, grad_values)


def solution(mesh):
    rows = P(("dp", "seq"), None)
    return jax.shard_map(
        shards,
        mesh=mesh,
        in_specs=(rows, rows, rows, P("dp"), rows),
        out_specs=(rows, rows, rows, rows),
        check_vma=False,
    )
```

```python
import functools
import math

import jax
import jax.numpy as jnp
from jax import lax
from jax.experimental import pallas as pl
from jax.experimental.pallas import tpu as pltpu
from jax.sharding import PartitionSpec as P

NEG_FILL = -1e30
LOG2_E = 1.4426950408889634


def ring_shift(value, steps):
    count = lax.axis_size("seq")
    return lax.ppermute(value, "seq", [(i, (i + steps) % count) for i in range(count)])


def dot_nt(left, right):
    return lax.dot_general(left, right, (((1,), (1,)), ((), ())), preferred_element_type=jnp.float32)


def dot_nn(left, right):
    return lax.dot_general(left, right, (((1,), (0,)), ((), ())), preferred_element_type=jnp.float32)


def head_lanes(head, width):
    return pl.ds(pl.multiple_of(head * width, width), width)


def take_rows(ref, group, pack, width):
    heads = [ref[:, head_lanes(group * pack + i, width)] for i in range(pack)]
    return jnp.concatenate(heads, axis=0)


def take_columns(ref, group, pack, width):
    heads = [ref[head_lanes(group * pack + i, width), :] for i in range(pack)]
    return jnp.concatenate(heads, axis=1)


def put_rows(ref, group, pack, width, value):
    tokens = value.shape[0] // pack
    for i in range(pack):
        ref[:, head_lanes(group * pack + i, width)] = value[i * tokens : (i + 1) * tokens]


def split_chain(lefts, rights, parts):
    step = lefts[0].shape[0] // parts
    sums = [None] * parts
    for left, right in zip(lefts, rights):
        for i in range(parts):
            part = dot_nn(left[i * step : (i + 1) * step], right)
            sums[i] = part if sums[i] is None else sums[i] + part
    return jnp.concatenate(sums, axis=0)


def split_nt(left, right, parts):
    step = left.shape[0] // parts
    return jnp.concatenate([dot_nt(left[i * step : (i + 1) * step], right) for i in range(parts)], axis=0)


def row_dots(left, right):
    return jnp.sum(left.astype(jnp.float32) * right.astype(jnp.float32), axis=1, keepdims=True)


def backward_slots(g, delta, q_t, g_t, weights, kv_refs, grad_ref, parts):
    tokens, width = kv_refs[0].shape[0] // 2, kv_refs[0].shape[1]
    steps = []
    for index, (w, kv_ref) in enumerate(zip(weights, kv_refs)):
        dp = split_nt(g, kv_ref[tokens:], parts)
        ds = (w.astype(jnp.float32) * (dp - delta)).astype(jnp.bfloat16)
        steps.append(ds)
        grad_ref[index, :width] += dot_nn(q_t, ds)
        grad_ref[index, width:] += dot_nn(g_t, w)
    return steps


def join_kernel(keys_ref, values_ref, own_ref, sems):
    tokens = keys_ref.shape[0]
    copies = [
        pltpu.make_async_copy(keys_ref, own_ref.at[pl.ds(0, tokens)], sems.at[0]),
        pltpu.make_async_copy(values_ref, own_ref.at[pl.ds(tokens, tokens)], sems.at[1]),
    ]
    for copy in copies:
        copy.start()
    for copy in copies:
        copy.wait()


def prepare_kernel(
    slot_count, lengths_ref, q_in, g_in, q_ref, g_ref, qt_ref, gt_ref, bias_ref, sems
):
    tokens = q_ref.shape[0]
    copies = [
        pltpu.make_async_copy(q_in, q_ref, sems.at[0]),
        pltpu.make_async_copy(g_in, g_ref, sems.at[1]),
    ]
    for copy in copies:
        copy.start()
    first = lax.axis_index("seq") * tokens
    row = lax.broadcasted_iota(jnp.int32, (tokens, tokens), 0)
    lane = lax.broadcasted_iota(jnp.int32, (tokens, tokens), 1)
    row_start = jnp.full((tokens, tokens), -first, jnp.int32)
    end = -first
    for document in range(lengths_ref.shape[0]):
        end = end + lengths_ref[document]
        row_start = jnp.where(row >= end, end, row_start)
    for slot in range(slot_count):
        visible = lane - slot * tokens >= row_start
        if slot == 0:
            visible = visible & (lane <= row)
        bias_ref[slot] = jnp.where(visible, 0.0, NEG_FILL)
    copies[0].wait()
    qt_ref[...] = q_ref[...].T
    copies[1].wait()
    gt_ref[...] = g_ref[...].T


def finish_kernel(score_scale, own_ref, *refs):
    part_refs, (keys_ref, values_ref) = refs[:-2], refs[-2:]
    width = keys_ref.shape[1]
    total = own_ref[0]
    for part_ref in part_refs:
        total = total + part_ref[...].astype(jnp.float32)
    keys_ref[...] = (score_scale * total[:width]).T.astype(jnp.bfloat16)
    values_ref[...] = total[width:].T.astype(jnp.bfloat16)


def forward_slots(q, bias_ref, first_slot, kv_refs, vext_ref, factor, pack, top):
    rows = q.shape[0]
    tokens = rows // pack
    scores = []
    for index, kv_ref in enumerate(kv_refs):
        part = dot_nt(q, kv_ref[:tokens]).reshape(pack, tokens, tokens)
        part = (part * factor + bias_ref[first_slot + index][None]).reshape(rows, tokens)
        scores.append(part)
    highest = scores[0]
    for part in scores[1:]:
        highest = jnp.maximum(highest, part)
    highest = jnp.broadcast_to(jnp.max(highest, axis=1, keepdims=True), (rows, q.shape[1]))
    if top is not None:
        highest = jnp.maximum(highest, top)
    level = jnp.concatenate([highest] * (tokens // q.shape[1]), axis=1)
    weights = [jnp.exp2(part - level).astype(jnp.bfloat16) for part in scores]
    total = split_chain(weights, [vext_ref[index] for index in range(len(kv_refs))], 2)
    return highest, weights, total


def extend_values(kv_refs, vext_ref):
    tokens, width = kv_refs[0].shape[0] // 2, kv_refs[0].shape[1]
    for index, kv_ref in enumerate(kv_refs):
        vext_ref[index, :, :width] = kv_ref[tokens:]
        vext_ref[index, :, width:] = jnp.ones((tokens, width), jnp.bfloat16)


def near_kernel(slots, pack, head_count, score_scale, *refs):
    bias_ref, q_ref = refs[:2]
    kv_refs = refs[2 : 2 + slots]
    kept_ref, total_ref, top_ref, vext_ref = refs[2 + slots :]
    width = q_ref.shape[1] // head_count
    rows = pack * q_ref.shape[0]
    extend_values(kv_refs, vext_ref)

    def one_group(group, carry):
        q = take_rows(q_ref, group, pack, width)
        top, weights, total = forward_slots(
            q, bias_ref, 0, kv_refs, vext_ref, score_scale * LOG2_E, pack, None
        )
        group_rows = pl.ds(pl.multiple_of(group * rows, rows), rows)
        for slot in range(slots):
            kept_ref[slot, group_rows] = weights[slot]
        total_ref[group_rows] = total
        top_ref[group_rows] = top
        return carry

    lax.fori_loop(0, head_count // pack, one_group, 0)


def far_kernel(first_slot, slots, pack, head_count, score_scale, *refs):
    bias_ref, q_ref, qt_ref, g_ref, gt_ref, total_ref, top_ref = refs[:7]
    kv_refs = refs[7 : 7 + slots]
    out_ref, step_ref, grad_out_ref, rate_ref, delta_ref, vext_ref, grad_ref = refs[7 + slots :]
    tokens = q_ref.shape[0]
    width = q_ref.shape[1] // head_count
    rows = pack * tokens
    extend_values(kv_refs, vext_ref)
    grad_ref[...] = jnp.zeros(grad_ref.shape, jnp.float32)

    def one_group(group, carry):
        group_rows = pl.ds(pl.multiple_of(group * rows, rows), rows)
        q = take_rows(q_ref, group, pack, width)
        g = take_rows(g_ref, group, pack, width)
        near_top = top_ref[group_rows]
        top, weights, total = forward_slots(
            q, bias_ref, first_slot, kv_refs, vext_ref, score_scale * LOG2_E, pack, near_top
        )
        shrink = jnp.exp2(near_top - top)
        near_total = total_ref[group_rows]
        inverse = 1.0 / (near_total[:, width:] * shrink + total[:, width:])
        out = ((near_total[:, :width] * shrink + total[:, :width]) * inverse).astype(jnp.bfloat16)
        put_rows(out_ref, group, pack, width, out)
        delta = row_dots(g, out)
        delta_ref[group_rows] = jnp.broadcast_to(delta, (rows, width))
        rate_ref[group_rows] = shrink * inverse
        inverse = jnp.concatenate([inverse] * (tokens // width), axis=1)
        weights = [(w.astype(jnp.float32) * inverse).astype(jnp.bfloat16) for w in weights]
        q_t = take_columns(qt_ref, group, pack, width)
        g_t = take_columns(gt_ref, group, pack, width)
        steps = backward_slots(g, delta, q_t, g_t, weights, kv_refs, grad_ref, 1)
        for slot in range(slots):
            step_ref[slot, group_rows] = steps[slot]
        return carry

    lax.fori_loop(0, head_count // pack, one_group, 0, unroll=True)
    grad_out_ref[...] = grad_ref[...].astype(grad_out_ref.dtype)


def later_kernel(first_slot, slots, pack, head_count, score_scale, *refs):
    qt_ref, g_ref, gt_ref, rate_ref, delta_ref, kept_ref = refs[:6]
    kv_refs = refs[6 : 6 + slots]
    last = first_slot == 0
    carried_ref, more_refs = refs[6 + slots], refs[7 + slots : -2]
    dq_ref, grad_ref = refs[-2:]
    tokens = g_ref.shape[0]
    width = g_ref.shape[1] // head_count
    rows = pack * tokens
    grad_ref[...] = jnp.zeros(grad_ref.shape, jnp.float32)

    def one_group(group, carry):
        g = take_rows(g_ref, group, pack, width)
        group_rows = pl.ds(pl.multiple_of(group * rows, rows), rows)
        delta = jnp.concatenate([delta_ref[group_rows]] * (tokens // width), axis=1)
        rate = jnp.concatenate([rate_ref[group_rows]] * (tokens // width), axis=1)
        weights = [
            (kept_ref[first_slot + index, group_rows].astype(jnp.float32) * rate).astype(jnp.bfloat16)
            for index in range(slots)
        ]
        q_t = take_columns(qt_ref, group, pack, width)
        g_t = take_columns(gt_ref, group, pack, width)
        steps = backward_slots(g, delta, q_t, g_t, weights, kv_refs, grad_ref, 2)
        if not last:
            steps = steps + [carried_ref[slot, group_rows] for slot in range(carried_ref.shape[0])]
        dq = split_chain(steps, [ref[:tokens] for ref in (*kv_refs, *more_refs)], 2)
        if last:
            dq = (dq + take_rows(carried_ref, group, pack, width)) * score_scale
        put_rows(dq_ref, group, pack, width, dq.astype(dq_ref.dtype))
        return carry

    lax.fori_loop(0, head_count // pack, one_group, 0)


VMEM = pl.BlockSpec(memory_space=pltpu.VMEM)
HBM = pl.BlockSpec(memory_space=pltpu.HBM)


def in_hbm(value):
    return pltpu.with_memory_space_constraint(value, pltpu.HBM)


def join_call(keys, values):
    return pl.pallas_call(
        join_kernel,
        out_shape=jax.ShapeDtypeStruct((2 * keys.shape[0], keys.shape[1]), keys.dtype),
        in_specs=[HBM] * 2,
        out_specs=VMEM,
        scratch_shapes=[pltpu.SemaphoreType.DMA((2,))],
        compiler_params=pltpu.CompilerParams(vmem_limit_bytes=1 << 20),
        name="join",
    )(in_hbm(keys), in_hbm(values))


def prepare_call(lengths, q, g, slot_count):
    tokens, lanes = q.shape
    return pl.pallas_call(
        functools.partial(prepare_kernel, slot_count),
        out_shape=(
            jax.ShapeDtypeStruct(q.shape, q.dtype),
            jax.ShapeDtypeStruct(g.shape, g.dtype),
            jax.ShapeDtypeStruct((lanes, tokens), q.dtype),
            jax.ShapeDtypeStruct((lanes, tokens), g.dtype),
            jax.ShapeDtypeStruct((slot_count, tokens, tokens), jnp.float32),
        ),
        in_specs=[pl.BlockSpec(memory_space=pltpu.SMEM), HBM, HBM],
        out_specs=(VMEM,) * 5,
        scratch_shapes=[pltpu.SemaphoreType.DMA((2,))],
        compiler_params=pltpu.CompilerParams(vmem_limit_bytes=2 << 20),
        name="prepare",
    )(in_hbm(lengths), in_hbm(q), in_hbm(g))


def finish_call(own, parts, score_scale, width):
    tokens = own.shape[2]
    shape = jax.ShapeDtypeStruct((tokens, width), jnp.bfloat16)
    return pl.pallas_call(
        functools.partial(finish_kernel, score_scale),
        out_shape=(shape, shape),
        in_specs=[VMEM] * (1 + len(parts)),
        out_specs=(VMEM,) * 2,
        compiler_params=pltpu.CompilerParams(vmem_limit_bytes=1 << 20),
        name="finish",
    )(own, *parts)


def near_call(bias, q, kvs, pack, head_count, score_scale):
    slots = len(kvs)
    tokens = q.shape[0]
    width = q.shape[1] // head_count
    rows = head_count * tokens
    return pl.pallas_call(
        functools.partial(near_kernel, slots, pack, head_count, score_scale),
        out_shape=(
            jax.ShapeDtypeStruct((slots, rows, tokens), jnp.bfloat16),
            jax.ShapeDtypeStruct((rows, 2 * width), jnp.float32),
            jax.ShapeDtypeStruct((rows, width), jnp.float32),
        ),
        in_specs=[VMEM] * (2 + slots),
        out_specs=(VMEM,) * 3,
        scratch_shapes=[pltpu.VMEM((slots, tokens, 2 * width), jnp.bfloat16)],
        compiler_params=pltpu.CompilerParams(vmem_limit_bytes=(slots + 1) * (4 << 20)),
        name="forward_near",
    )(bias, q, *kvs)


def far_call(bias, q, qt, g, gt, total, top, kvs, first_slot, pack, head_count, score_scale):
    slots = len(kvs)
    tokens = q.shape[0]
    width = q.shape[1] // head_count
    rows = head_count * tokens
    return pl.pallas_call(
        functools.partial(far_kernel, first_slot, slots, pack, head_count, score_scale),
        out_shape=(
            jax.ShapeDtypeStruct(q.shape, jnp.bfloat16),
            jax.ShapeDtypeStruct((slots, rows, tokens), jnp.bfloat16),
            jax.ShapeDtypeStruct((slots, 2 * width, tokens), jnp.bfloat16),
            jax.ShapeDtypeStruct((rows, width), jnp.float32),
            jax.ShapeDtypeStruct((rows, width), jnp.float32),
        ),
        in_specs=[VMEM] * (7 + slots),
        out_specs=(VMEM,) * 5,
        scratch_shapes=[
            pltpu.VMEM((slots, tokens, 2 * width), jnp.bfloat16),
            pltpu.VMEM((slots, 2 * width, tokens), jnp.float32),
        ],
        compiler_params=pltpu.CompilerParams(vmem_limit_bytes=(slots + 1) * (7 << 20)),
        name="forward_far",
    )(bias, q, qt, g, gt, total, top, *kvs)


def later_call(qt, g, gt, rate, delta, kept, kvs, carried, more, first_slot, pack, head_count, score_scale):
    slots = len(kvs)
    tokens = g.shape[0]
    width = g.shape[1] // head_count
    last = first_slot == 0
    return pl.pallas_call(
        functools.partial(later_kernel, first_slot, slots, pack, head_count, score_scale),
        out_shape=(
            jax.ShapeDtypeStruct(g.shape, jnp.bfloat16 if last else jnp.float32),
            jax.ShapeDtypeStruct((slots, 2 * width, tokens), jnp.float32),
        ),
        in_specs=[VMEM] * (7 + slots + len(more)),
        out_specs=(VMEM,) * 2,
        compiler_params=pltpu.CompilerParams(vmem_limit_bytes=(slots + len(more) + 1) * (4 << 20)),
        name="backward_last" if last else "backward_near",
    )(qt, g, gt, rate, delta, kept, *kvs, carried, *more)


def shards(queries, keys, values, lengths, grad_out):
    width = keys.shape[1]
    head_count = queries.shape[1] // width
    reach = min(8, lax.axis_size("seq") // 2)
    score_scale = 1.0 / math.sqrt(width)
    pack_a = math.gcd(8, head_count)
    pack_f = math.gcd(8, head_count)
    pack_2 = math.gcd(8, head_count)
    pack_3 = math.gcd(16, head_count)

    near = reach // 2 + 1
    own = join_call(keys, values)
    two = ring_shift(own, 2)
    one = ring_shift(own, 1)
    queries, grad_out, queries_t, grads_t, bias = prepare_call(
        lengths, queries, grad_out, reach + 1
    )
    two, bias = lax.optimization_barrier((two, bias))
    window = [own, one, two]
    if reach > 2:
        window += [ring_shift(two, 1), ring_shift(two, 2)]
    while len(window) <= reach:
        shift = len(window) - 1
        window += [ring_shift(part, shift) for part in window[1:]]
    window = window[: reach + 1]

    kept, total, top = near_call(bias, queries, window[:near], pack_a, head_count, score_scale)
    out, far_steps, far_grads, rate, delta = far_call(
        bias, queries, queries_t, grad_out, grads_t, total, top, window[near:], near, pack_f, head_count, score_scale
    )
    moved = ring_shift(far_grads, -(reach // 2))
    shared = (queries_t, grad_out, grads_t, rate, delta, kept)
    dq, near_grads = later_call(
        *shared, window[1:near], far_steps, window[near:], 1, pack_2, head_count, score_scale
    )
    near_grads = (near_grads + moved.astype(jnp.float32)).astype(jnp.bfloat16)
    while near_grads.shape[0] > 2:
        half = near_grads.shape[0] // 2
        back = ring_shift(near_grads[half:], -half)
        near_grads = (near_grads[:half].astype(jnp.float32) + back.astype(jnp.float32)).astype(jnp.bfloat16)
    received = [ring_shift(near_grads[i], -1 - i) for i in range(near_grads.shape[0])]
    dq, own_grads = later_call(
        *shared, window[:1], dq, [], 0, pack_3, head_count, score_scale
    )
    grad_keys, grad_values = finish_call(own_grads, received, score_scale, width)
    return (out, dq, grad_keys, grad_values)


def solution(mesh):
    rows = P(("dp", "seq"), None)
    return jax.shard_map(
        shards,
        mesh=mesh,
        in_specs=(rows, rows, rows, P("dp"), rows),
        out_specs=(rows, rows, rows, rows),
        check_vma=False,
    )
```

```python
import functools
import math

import jax
import jax.numpy as jnp
from jax import lax
from jax.experimental import pallas as pl
from jax.experimental.pallas import tpu as pltpu
from jax.sharding import PartitionSpec as P

NEG_FILL = -1e30
LOG2_E = 1.4426950408889634


def ring_shift(value, steps):
    count = lax.axis_size("seq")
    return lax.ppermute(value, "seq", [(i, (i + steps) % count) for i in range(count)])


def dot_nt(left, right):
    return lax.dot_general(left, right, (((1,), (1,)), ((), ())), preferred_element_type=jnp.float32)


def dot_nn(left, right):
    return lax.dot_general(left, right, (((1,), (0,)), ((), ())), preferred_element_type=jnp.float32)


def head_lanes(head, width):
    return pl.ds(pl.multiple_of(head * width, width), width)


def take_rows(ref, group, pack, width):
    heads = [ref[:, head_lanes(group * pack + i, width)] for i in range(pack)]
    return jnp.concatenate(heads, axis=0)


def take_columns(ref, group, pack, width):
    heads = [ref[head_lanes(group * pack + i, width), :] for i in range(pack)]
    return jnp.concatenate(heads, axis=1)


def put_rows(ref, group, pack, width, value):
    tokens = value.shape[0] // pack
    for i in range(pack):
        ref[:, head_lanes(group * pack + i, width)] = value[i * tokens : (i + 1) * tokens]


def split_chain(lefts, rights, parts):
    step = lefts[0].shape[0] // parts
    sums = [None] * parts
    for left, right in zip(lefts, rights):
        for i in range(parts):
            part = dot_nn(left[i * step : (i + 1) * step], right)
            sums[i] = part if sums[i] is None else sums[i] + part
    return jnp.concatenate(sums, axis=0)


def split_nt(left, right, parts):
    step = left.shape[0] // parts
    return jnp.concatenate([dot_nt(left[i * step : (i + 1) * step], right) for i in range(parts)], axis=0)


def row_dots(left, right):
    return jnp.sum(left.astype(jnp.float32) * right.astype(jnp.float32), axis=1, keepdims=True)


def backward_slots(g, delta, q_t, g_t, weights, kv_refs, grad_ref, parts):
    tokens, width = kv_refs[0].shape[0] // 2, kv_refs[0].shape[1]
    steps = []
    for index, (w, kv_ref) in enumerate(zip(weights, kv_refs)):
        dp = split_nt(g, kv_ref[tokens:], parts)
        ds = (w.astype(jnp.float32) * (dp - delta)).astype(jnp.bfloat16)
        steps.append(ds)
        grad_ref[index, :width] += dot_nn(q_t, ds)
        grad_ref[index, width:] += dot_nn(g_t, w)
    return steps


def join_kernel(keys_ref, values_ref, own_ref, sems):
    tokens = keys_ref.shape[0]
    copies = [
        pltpu.make_async_copy(keys_ref, own_ref.at[pl.ds(0, tokens)], sems.at[0]),
        pltpu.make_async_copy(values_ref, own_ref.at[pl.ds(tokens, tokens)], sems.at[1]),
    ]
    for copy in copies:
        copy.start()
    for copy in copies:
        copy.wait()


def prepare_kernel(
    slot_count, lengths_ref, q_in, g_in, q_ref, g_ref, qt_ref, gt_ref, bias_ref, sems
):
    tokens = q_ref.shape[0]
    copies = [
        pltpu.make_async_copy(q_in, q_ref, sems.at[0]),
        pltpu.make_async_copy(g_in, g_ref, sems.at[1]),
    ]
    for copy in copies:
        copy.start()
    first = lax.axis_index("seq") * tokens
    row = lax.broadcasted_iota(jnp.int32, (tokens, tokens), 0)
    lane = lax.broadcasted_iota(jnp.int32, (tokens, tokens), 1)
    row_start = jnp.full((tokens, tokens), -first, jnp.int32)
    end = -first
    for document in range(lengths_ref.shape[0]):
        end = end + lengths_ref[document]
        row_start = jnp.where(row >= end, end, row_start)
    for slot in range(slot_count):
        visible = lane - slot * tokens >= row_start
        if slot == 0:
            visible = visible & (lane <= row)
        bias_ref[slot] = jnp.where(visible, 0.0, NEG_FILL)
    copies[0].wait()
    qt_ref[...] = q_ref[...].T
    copies[1].wait()
    gt_ref[...] = g_ref[...].T


def finish_kernel(score_scale, own_ref, *refs):
    part_refs, (keys_ref, values_ref) = refs[:-2], refs[-2:]
    width = keys_ref.shape[1]
    total = own_ref[0] + pick_back(part_refs[0][...], part_refs[1][...], 2)
    for part_ref in part_refs[2:]:
        total = total + part_ref[...].astype(jnp.float32)
    keys_ref[...] = (score_scale * total[:width]).T.astype(jnp.bfloat16)
    values_ref[...] = total[width:].T.astype(jnp.bfloat16)


def forward_slots(q, bias_ref, first_slot, kv_refs, vext_ref, factor, pack, top):
    rows = q.shape[0]
    tokens = rows // pack
    scores = []
    for index, kv_ref in enumerate(kv_refs):
        part = dot_nt(q, kv_ref[:tokens]).reshape(pack, tokens, tokens)
        part = (part * factor + bias_ref[first_slot + index][None]).reshape(rows, tokens)
        scores.append(part)
    highest = scores[0]
    for part in scores[1:]:
        highest = jnp.maximum(highest, part)
    highest = jnp.broadcast_to(jnp.max(highest, axis=1, keepdims=True), (rows, q.shape[1]))
    if top is not None:
        highest = jnp.maximum(highest, top)
    level = jnp.concatenate([highest] * (tokens // q.shape[1]), axis=1)
    weights = [jnp.exp2(part - level).astype(jnp.bfloat16) for part in scores]
    total = split_chain(weights, [vext_ref[index] for index in range(len(kv_refs))], 2)
    return highest, weights, total


def extend_values(kv_refs, vext_ref):
    tokens, width = kv_refs[0].shape[0] // 2, kv_refs[0].shape[1]
    for index, kv_ref in enumerate(kv_refs):
        vext_ref[index, :, :width] = kv_ref[tokens:]
        vext_ref[index, :, width:] = jnp.ones((tokens, width), jnp.bfloat16)


def near_kernel(slots, pack, head_count, score_scale, *refs):
    bias_ref, q_ref = refs[:2]
    kv_refs = refs[2 : 2 + slots]
    kept_ref, total_ref, top_ref, vext_ref = refs[2 + slots :]
    width = q_ref.shape[1] // head_count
    rows = pack * q_ref.shape[0]
    extend_values(kv_refs, vext_ref)

    def one_group(group, carry):
        q = take_rows(q_ref, group, pack, width)
        top, weights, total = forward_slots(
            q, bias_ref, 0, kv_refs, vext_ref, score_scale * LOG2_E, pack, None
        )
        group_rows = pl.ds(pl.multiple_of(group * rows, rows), rows)
        for slot in range(slots):
            kept_ref[slot, group_rows] = weights[slot]
        total_ref[group_rows] = total
        top_ref[group_rows] = top
        return carry

    lax.fori_loop(0, head_count // pack, one_group, 0)


def far_kernel(first_slot, slots, pack, head_count, score_scale, *refs):
    bias_ref, q_ref, qt_ref, g_ref, gt_ref, total_ref, top_ref = refs[:7]
    kv_refs = refs[7 : 7 + slots]
    out_ref, step_ref, grad_out_ref, rate_ref, delta_ref, vext_ref, grad_ref = refs[7 + slots :]
    tokens = q_ref.shape[0]
    width = q_ref.shape[1] // head_count
    rows = pack * tokens
    extend_values(kv_refs, vext_ref)
    grad_ref[...] = jnp.zeros(grad_ref.shape, jnp.float32)

    def one_group(group, carry):
        group_rows = pl.ds(pl.multiple_of(group * rows, rows), rows)
        q = take_rows(q_ref, group, pack, width)
        g = take_rows(g_ref, group, pack, width)
        near_top = top_ref[group_rows]
        top, weights, total = forward_slots(
            q, bias_ref, first_slot, kv_refs, vext_ref, score_scale * LOG2_E, pack, near_top
        )
        shrink = jnp.exp2(near_top - top)
        near_total = total_ref[group_rows]
        inverse = 1.0 / (near_total[:, width:] * shrink + total[:, width:])
        out = ((near_total[:, :width] * shrink + total[:, :width]) * inverse).astype(jnp.bfloat16)
        put_rows(out_ref, group, pack, width, out)
        delta = row_dots(g, out)
        delta_ref[group_rows] = jnp.broadcast_to(delta, (rows, width))
        rate_ref[group_rows] = shrink * inverse
        inverse = jnp.concatenate([inverse] * (tokens // width), axis=1)
        weights = [(w.astype(jnp.float32) * inverse).astype(jnp.bfloat16) for w in weights]
        q_t = take_columns(qt_ref, group, pack, width)
        g_t = take_columns(gt_ref, group, pack, width)
        steps = backward_slots(g, delta, q_t, g_t, weights, kv_refs, grad_ref, 1)
        for slot in range(slots):
            step_ref[slot, group_rows] = steps[slot]
        return carry

    lax.fori_loop(0, head_count // pack, one_group, 0, unroll=True)
    grad_out_ref[...] = grad_ref[...].astype(grad_out_ref.dtype)


def later_kernel(first_slot, slots, pack, head_count, score_scale, *refs):
    qt_ref, g_ref, gt_ref, rate_ref, delta_ref, kept_ref = refs[:6]
    kv_refs = refs[6 : 6 + slots]
    last = first_slot == 0
    carried_ref, more_refs = refs[6 + slots], refs[7 + slots : -2]
    dq_ref, grad_ref = refs[-2:]
    tokens = g_ref.shape[0]
    width = g_ref.shape[1] // head_count
    rows = pack * tokens
    grad_ref[...] = jnp.zeros(grad_ref.shape, jnp.float32)

    def one_group(group, carry):
        g = take_rows(g_ref, group, pack, width)
        group_rows = pl.ds(pl.multiple_of(group * rows, rows), rows)
        delta = jnp.concatenate([delta_ref[group_rows]] * (tokens // width), axis=1)
        rate = jnp.concatenate([rate_ref[group_rows]] * (tokens // width), axis=1)
        weights = [
            (kept_ref[first_slot + index, group_rows].astype(jnp.float32) * rate).astype(jnp.bfloat16)
            for index in range(slots)
        ]
        q_t = take_columns(qt_ref, group, pack, width)
        g_t = take_columns(gt_ref, group, pack, width)
        steps = backward_slots(g, delta, q_t, g_t, weights, kv_refs, grad_ref, 2)
        if not last:
            steps = steps + [carried_ref[slot, group_rows] for slot in range(carried_ref.shape[0])]
        dq = split_chain(steps, [ref[:tokens] for ref in (*kv_refs, *more_refs)], 2)
        if last:
            dq = (dq + take_rows(carried_ref, group, pack, width)) * score_scale
        put_rows(dq_ref, group, pack, width, dq.astype(dq_ref.dtype))
        return carry

    lax.fori_loop(0, head_count // pack, one_group, 0)


VMEM = pl.BlockSpec(memory_space=pltpu.VMEM)
HBM = pl.BlockSpec(memory_space=pltpu.HBM)


def in_hbm(value):
    return pltpu.with_memory_space_constraint(value, pltpu.HBM)


def join_call(keys, values):
    return pl.pallas_call(
        join_kernel,
        out_shape=jax.ShapeDtypeStruct((2 * keys.shape[0], keys.shape[1]), keys.dtype),
        in_specs=[HBM] * 2,
        out_specs=VMEM,
        scratch_shapes=[pltpu.SemaphoreType.DMA((2,))],
        compiler_params=pltpu.CompilerParams(vmem_limit_bytes=1 << 20),
        name="join",
    )(in_hbm(keys), in_hbm(values))


def prepare_call(lengths, q, g, slot_count):
    tokens, lanes = q.shape
    return pl.pallas_call(
        functools.partial(prepare_kernel, slot_count),
        out_shape=(
            jax.ShapeDtypeStruct(q.shape, q.dtype),
            jax.ShapeDtypeStruct(g.shape, g.dtype),
            jax.ShapeDtypeStruct((lanes, tokens), q.dtype),
            jax.ShapeDtypeStruct((lanes, tokens), g.dtype),
            jax.ShapeDtypeStruct((slot_count, tokens, tokens), jnp.float32),
        ),
        in_specs=[pl.BlockSpec(memory_space=pltpu.SMEM), HBM, HBM],
        out_specs=(VMEM,) * 5,
        scratch_shapes=[pltpu.SemaphoreType.DMA((2,))],
        compiler_params=pltpu.CompilerParams(vmem_limit_bytes=2 << 20),
        name="prepare",
    )(in_hbm(lengths), in_hbm(q), in_hbm(g))


def finish_call(own, parts, score_scale, width):
    tokens = own.shape[2]
    shape = jax.ShapeDtypeStruct((tokens, width), jnp.bfloat16)
    return pl.pallas_call(
        functools.partial(finish_kernel, score_scale),
        out_shape=(shape, shape),
        in_specs=[VMEM] * (1 + len(parts)),
        out_specs=(VMEM,) * 2,
        compiler_params=pltpu.CompilerParams(vmem_limit_bytes=1 << 20),
        name="finish",
    )(own, *parts)


def near_call(bias, q, kvs, pack, head_count, score_scale):
    slots = len(kvs)
    tokens = q.shape[0]
    width = q.shape[1] // head_count
    rows = head_count * tokens
    return pl.pallas_call(
        functools.partial(near_kernel, slots, pack, head_count, score_scale),
        out_shape=(
            jax.ShapeDtypeStruct((slots, rows, tokens), jnp.bfloat16),
            jax.ShapeDtypeStruct((rows, 2 * width), jnp.float32),
            jax.ShapeDtypeStruct((rows, width), jnp.float32),
        ),
        in_specs=[VMEM] * (2 + slots),
        out_specs=(VMEM,) * 3,
        scratch_shapes=[pltpu.VMEM((slots, tokens, 2 * width), jnp.bfloat16)],
        compiler_params=pltpu.CompilerParams(vmem_limit_bytes=(slots + 1) * (4 << 20)),
        name="forward_near",
    )(bias, q, *kvs)


def far_call(bias, q, qt, g, gt, total, top, kvs, first_slot, pack, head_count, score_scale):
    slots = len(kvs)
    tokens = q.shape[0]
    width = q.shape[1] // head_count
    rows = head_count * tokens
    return pl.pallas_call(
        functools.partial(far_kernel, first_slot, slots, pack, head_count, score_scale),
        out_shape=(
            jax.ShapeDtypeStruct(q.shape, jnp.bfloat16),
            jax.ShapeDtypeStruct((slots, rows, tokens), jnp.bfloat16),
            jax.ShapeDtypeStruct((slots, 2 * width, tokens), jnp.bfloat16),
            jax.ShapeDtypeStruct((rows, width), jnp.float32),
            jax.ShapeDtypeStruct((rows, width), jnp.float32),
        ),
        in_specs=[VMEM] * (7 + slots),
        out_specs=(VMEM,) * 5,
        scratch_shapes=[
            pltpu.VMEM((slots, tokens, 2 * width), jnp.bfloat16),
            pltpu.VMEM((slots, 2 * width, tokens), jnp.float32),
        ],
        compiler_params=pltpu.CompilerParams(vmem_limit_bytes=(slots + 1) * (7 << 20)),
        name="forward_far",
    )(bias, q, qt, g, gt, total, top, *kvs)


def later_call(qt, g, gt, rate, delta, kept, kvs, carried, more, first_slot, pack, head_count, score_scale):
    slots = len(kvs)
    tokens = g.shape[0]
    width = g.shape[1] // head_count
    last = first_slot == 0
    return pl.pallas_call(
        functools.partial(later_kernel, first_slot, slots, pack, head_count, score_scale),
        out_shape=(
            jax.ShapeDtypeStruct(g.shape, jnp.bfloat16 if last else jnp.float32),
            jax.ShapeDtypeStruct((slots, 2 * width, tokens), jnp.float32),
        ),
        in_specs=[VMEM] * (7 + slots + len(more)),
        out_specs=(VMEM,) * 2,
        compiler_params=pltpu.CompilerParams(vmem_limit_bytes=(slots + len(more) + 1) * (4 << 20)),
        name="backward_last" if last else "backward_near",
    )(qt, g, gt, rate, delta, kept, *kvs, carried, *more)


def swap_partners(count, steps, offset):
    partners = []
    for i in range(count):
        j = i + steps if (i // steps) % 2 == offset else i - steps
        partners.append((i, j if 0 <= j < count else i ^ 1))
    return partners


def swap_back(value, steps):
    count = lax.axis_size("seq")
    return [lax.ppermute(value, "seq", swap_partners(count, steps, offset)) for offset in range(2)]


def pick_back(first, second, steps):
    rank, count = lax.axis_index("seq"), lax.axis_size("seq")
    odd = jnp.full(first.shape, (rank // steps) % 2, jnp.int32) == 1
    inside = jnp.full(first.shape, rank + steps, jnp.int32) < count
    moved = jnp.where(odd, second, first).astype(jnp.float32)
    return jnp.where(inside, moved, 0.0)


def merge_kernel(steps, near_ref, first_ref, second_ref, *out_refs):
    for slot, out_ref in enumerate(out_refs):
        moved = pick_back(first_ref[slot], second_ref[slot], steps)
        out_ref[...] = (near_ref[slot].astype(jnp.float32) + moved).astype(jnp.bfloat16)


def merge_call(near_grads, moved, steps):
    slots, *shape = near_grads.shape
    return pl.pallas_call(
        functools.partial(merge_kernel, steps),
        out_shape=(jax.ShapeDtypeStruct(shape, jnp.bfloat16),) * slots,
        in_specs=[VMEM] * 3,
        out_specs=(VMEM,) * slots,
        compiler_params=pltpu.CompilerParams(vmem_limit_bytes=1 << 20),
        name="merge",
    )(near_grads, *moved)


def choose_kernel(steps, first_ref, second_ref, out_ref):
    odd = (lax.axis_index("seq") // steps) % 2 == 1

    @pl.when(odd)
    def _():
        out_ref[...] = first_ref[...]

    @pl.when(jnp.logical_not(odd))
    def _():
        out_ref[...] = second_ref[...]


def swap_forward(value, steps):
    moved = swap_back(value, steps)
    return pl.pallas_call(
        functools.partial(choose_kernel, steps),
        out_shape=jax.ShapeDtypeStruct(value.shape, value.dtype),
        in_specs=[VMEM] * 2,
        out_specs=VMEM,
        compiler_params=pltpu.CompilerParams(vmem_limit_bytes=1 << 20),
        name="choose",
    )(*moved)


def shards(queries, keys, values, lengths, grad_out):
    width = keys.shape[1]
    head_count = queries.shape[1] // width
    reach = min(8, lax.axis_size("seq") // 2)
    score_scale = 1.0 / math.sqrt(width)
    pack_a = math.gcd(8, head_count)
    pack_f = math.gcd(8, head_count)
    pack_2 = math.gcd(8, head_count)
    pack_3 = math.gcd(16, head_count)

    near = reach // 2 + 1
    own = join_call(keys, values)
    two = swap_forward(own, 2)
    one = ring_shift(own, 1)
    queries, grad_out, queries_t, grads_t, bias = prepare_call(
        lengths, queries, grad_out, reach + 1
    )
    two, bias = lax.optimization_barrier((two, bias))
    window = [own, one, two]
    if reach > 2:
        window += [ring_shift(two, 1), ring_shift(two, 2)]
    while len(window) <= reach:
        shift = len(window) - 1
        window += [ring_shift(part, shift) for part in window[1:]]
    window = window[: reach + 1]

    kept, total, top = near_call(bias, queries, window[:near], pack_a, head_count, score_scale)
    out, far_steps, far_grads, rate, delta = far_call(
        bias, queries, queries_t, grad_out, grads_t, total, top, window[near:], near, pack_f, head_count, score_scale
    )
    moved = swap_back(far_grads, reach // 2)
    shared = (queries_t, grad_out, grads_t, rate, delta, kept)
    dq, near_grads = later_call(
        *shared, window[1:near], far_steps, window[near:], 1, pack_2, head_count, score_scale
    )
    parts = merge_call(near_grads, moved, reach // 2)
    while len(parts) > 2:
        half = len(parts) // 2
        moved = swap_back(jnp.stack(parts[half:]), half)
        parts = merge_call(jnp.stack(parts[:half]), moved, half)
    received = [*swap_back(parts[1], 2), ring_shift(parts[0], -1)]
    dq, own_grads = later_call(
        *shared, window[:1], dq, [], 0, pack_3, head_count, score_scale
    )
    grad_keys, grad_values = finish_call(own_grads, received, score_scale, width)
    return (out, dq, grad_keys, grad_values)


def solution(mesh):
    rows = P(("dp", "seq"), None)
    return jax.shard_map(
        shards,
        mesh=mesh,
        in_specs=(rows, rows, rows, P("dp"), rows),
        out_specs=(rows, rows, rows, rows),
        check_vma=False,
    )
```
